1024 devices in a mesh: dp: 8 (over z_lo, core), ctx: 8 (over y), head: 16 (over x, z_hi).
Axes of the slice: x: 8, y: 8, z: 8 (z_hi: 2, z_lo: 4; z = z_hi * 4 + z_lo), core: 2. Of those that a mesh axis runs over, the one named last changes fastest.
Arguments:
- latent: bfloat16 [8, 1024, 512], P('dp', 'ctx'), may hold values from -6 to 6
- rope: bfloat16 [8, 1024, 64], P('dp', 'ctx'), may hold values from -6 to 6
- query: bfloat16 [8, 1024, 12288], P('dp', 'ctx', 'head'), may hold values from -9 to 9
- grad_out: bfloat16 [8, 1024, 8192], P('dp', 'ctx', 'head'), may hold values from -6 to 6
- attn_out: bfloat16 [8, 1024, 8192], P('dp', 'ctx', 'head'), may hold values from -40 to 40
- lse: float32 [8, 64, 1024], P('dp', 'head', 'ctx'), may hold values from -100 to 100, as said below
- positions: int32 [8, 1024], P('dp'), may hold values from 0 to 1023, as said below
- w_uk: bfloat16 [512, 8192], P(None, 'head'), may hold values from -2 to 2
- w_uv: bfloat16 [512, 8192], P(None, 'head'), may hold values from -2 to 2
Outputs:
- grad_query: bfloat16 [8, 1024, 12288], P('dp', 'ctx', 'head')
- grad_latent: float32 [8, 1024, 512], P('dp', 'ctx')
- grad_rope: float32 [8, 1024, 64], P('dp', 'ctx')
- grad_wuk: bfloat16 [512, 8192], P(('dp', 'ctx'), 'head')
- grad_wuv: bfloat16 [512, 8192], P(('dp', 'ctx'), 'head')
The draws below stay inside these ranges and needn't reach their ends.
Inputs may be any that keep to these rules, and one draw needn't show every extreme that they name: Each sequence's row is a permutation of 0 to 1023 made of runs of 64 consecutive positions, each run filling an aligned run of 64 rows in rising order; which run goes to which rows is drawn. lse[h, i] is the log of the sum of exp(scores[i, j]) over the keys j with positions[j] <= positions[i].
All inputs are finite; a program needn't handle non-finite values.
Results may differ from the reference program's by a relative error of at most 0.02.
Values may be sent and summed in bfloat16 or wider, within the bound.
A program may use at most 64 MiB of HBM per device.

```python
import math
import jax
import jax.numpy as jnp
from jax import lax

DL = 512
DR = 64
DN = 128
DV = 128
HEADS = 64
HALF = 64
TOKENS = 1024
SEQS = 8


MASKED = -1e+30


def draw_order(key):
    block_count = TOKENS // HALF

    def one_sequence(index):
        shuffled = jax.random.permutation(jax.random.fold_in(key, 5000 + index), block_count).astype(jnp.int32)
        token_index = jnp.arange(TOKENS, dtype=jnp.int32)
        return (shuffled[token_index // HALF] * HALF + token_index % HALF).astype(jnp.int32)
    return jax.vmap(one_sequence)(jnp.arange(SEQS, dtype=jnp.int32))


def make_floats(key):
    streams = [jax.random.fold_in(key, 900 + index) for index in range(8)]
    latent = jnp.clip(jax.random.normal(streams[0], (SEQS, TOKENS, DL), jnp.float32), -6.0, 6.0)
    query = jnp.clip(1.4 * jax.random.normal(streams[2], (SEQS, TOKENS, HEADS * (DN + DR)), jnp.float32), -8.0, 8.0)
    grad_out = jnp.clip(jax.random.normal(streams[5], (SEQS, TOKENS, HEADS * DV), jnp.float32), -6.0, 6.0)
    rope = jnp.clip(jax.random.normal(streams[1], (SEQS, TOKENS, DR), jnp.float32), -6.0, 6.0)
    w_uk = jnp.clip(jax.random.normal(streams[3], (DL, HEADS * DN), jnp.float32), -6.0, 6.0) / math.sqrt(DL)
    w_uv = jnp.clip(jax.random.normal(streams[4], (DL, HEADS * DV), jnp.float32), -6.0, 6.0) / math.sqrt(DL)
    return (latent.astype(jnp.bfloat16), rope.astype(jnp.bfloat16), query.astype(jnp.bfloat16), grad_out.astype(jnp.bfloat16), w_uk.astype(jnp.bfloat16), w_uv.astype(jnp.bfloat16))


def forward_pass(key):
    latent, rope, query, grad_out, w_uk, w_uv = make_floats(key)
    seq_orders = draw_order(jax.random.fold_in(key, 77))
    score_scale = 1.0 / math.sqrt(DN + DR)

    def one_sequence(item):
        seq_latent, seq_rope, seq_query, seq_order = item
        nope = jnp.dot(seq_latent, w_uk, preferred_element_type=jnp.float32).astype(jnp.bfloat16)
        nope = nope.reshape(TOKENS, HEADS, DN).transpose(1, 0, 2)
        value_rows = jnp.dot(seq_latent, w_uv, preferred_element_type=jnp.float32).astype(jnp.bfloat16)
        value_rows = value_rows.reshape(TOKENS, HEADS, DV).transpose(1, 0, 2)
        queries = seq_query.reshape(TOKENS, HEADS, DN + DR).transpose(1, 0, 2)
        allowed = seq_order[None, :] <= seq_order[:, None]

        def one_head(part_item):
            head_query, head_nope, head_values = part_item
            head_keys = jnp.concatenate([head_nope, seq_rope], axis=1)
            scores = jnp.dot(head_query, head_keys.T, preferred_element_type=jnp.float32) * score_scale
            scores = jnp.where(allowed, scores, MASKED)
            top_score = jnp.max(scores, axis=1, keepdims=True)
            expo = jnp.exp(scores - top_score)
            total = jnp.sum(expo, axis=1, keepdims=True)
            mixed = jnp.dot(expo / total, head_values.astype(jnp.float32), precision=lax.Precision.HIGHEST)
            return (mixed, top_score[:, 0] + jnp.log(total[:, 0]))
        mixed, log_total = lax.map(one_head, (queries, nope, value_rows))
        return (mixed.transpose(1, 0, 2).reshape(TOKENS, HEADS * DV), log_total)
    return lax.map(one_sequence, (latent, rope, query, seq_orders))


def draw_latent(key, part):
    return make_floats(key)[0]


def draw_rope(key, part):
    return make_floats(key)[1]


def draw_query(key, part):
    return make_floats(key)[2]


def draw_grad_out(key, part):
    return make_floats(key)[3]


def draw_w_uk(key, part):
    return make_floats(key)[4]


def draw_w_uv(key, part):
    return make_floats(key)[5]


def draw_attn_out(key, part):
    return forward_pass(key)[0].astype(jnp.bfloat16)


def draw_lse(key, part):
    return forward_pass(key)[1].astype(jnp.float32)


def draw_positions(key, part):
    return draw_order(jax.random.fold_in(key, 77))


def setup_inputs(seed: int = 0) -> dict:
    streams_of = jax.random.split(jax.random.key(seed), 10)
    return {
        "latent": draw_latent(jax.random.fold_in(streams_of[9], 71), 0),
        "rope": draw_rope(jax.random.fold_in(streams_of[9], 71), 0),
        "query": draw_query(jax.random.fold_in(streams_of[9], 71), 0),
        "grad_out": draw_grad_out(jax.random.fold_in(streams_of[9], 71), 0),
        "attn_out": draw_attn_out(jax.random.fold_in(streams_of[9], 71), 0),
        "lse": draw_lse(jax.random.fold_in(streams_of[9], 71), 0),
        "positions": draw_positions(jax.random.fold_in(streams_of[9], 71), 0),
        "w_uk": draw_w_uk(jax.random.fold_in(streams_of[9], 71), 0),
        "w_uv": draw_w_uv(jax.random.fold_in(streams_of[9], 71), 0),
    }


MASKED = -1e+30

def sequence_grads(latent, rope, query, grad_out, attn_out, lse, positions, w_uk, w_uv):
    score_scale = 1.0 / math.sqrt(DN + DR)
    keys_nope = jnp.dot(latent, w_uk, preferred_element_type=jnp.float32).astype(jnp.bfloat16)
    keys_nope = keys_nope.reshape(TOKENS, HEADS, DN).transpose(1, 0, 2)
    values = jnp.dot(latent, w_uv, preferred_element_type=jnp.float32).astype(jnp.bfloat16)
    values = values.reshape(TOKENS, HEADS, DV).transpose(1, 0, 2)
    queries = query.reshape(TOKENS, HEADS, DN + DR).transpose(1, 0, 2)
    grads = grad_out.reshape(TOKENS, HEADS, DV).transpose(1, 0, 2)
    outputs = attn_out.reshape(TOKENS, HEADS, DV).transpose(1, 0, 2)
    allowed = positions[None, :] <= positions[:, None]

    def per_head(item):
        head_query, head_nope, head_values, head_grads, head_outputs, head_lse = item
        head_keys = jnp.concatenate([head_nope, rope], axis=1)
        scores = jnp.dot(head_query, head_keys.T, preferred_element_type=jnp.float32) * score_scale
        weights = jnp.exp(jnp.where(allowed, scores - head_lse[:, None], MASKED))
        dots = jnp.dot(head_grads, head_values.T, preferred_element_type=jnp.float32)
        delta = lax.optimization_barrier(jnp.sum(head_grads.astype(jnp.float32) * head_outputs.astype(jnp.float32), axis=1))
        score_grad = (weights * (dots - delta[:, None]) * score_scale).astype(jnp.bfloat16)
        weights_b = weights.astype(jnp.bfloat16)
        query_grad = jnp.dot(score_grad, head_keys, preferred_element_type=jnp.float32)
        key_grad = jnp.dot(score_grad.T, head_query, preferred_element_type=jnp.float32)
        value_grad = jnp.dot(weights_b.T, head_grads, preferred_element_type=jnp.float32)
        return (query_grad, key_grad, value_grad)
    query_grad, key_grad, value_grad = lax.map(per_head, (queries, keys_nope, values, grads, outputs, lse))
    query_out = query_grad.transpose(1, 0, 2).reshape(TOKENS, HEADS * (DN + DR)).astype(jnp.bfloat16)
    key_nope = key_grad[:, :, :DN].transpose(1, 0, 2).reshape(TOKENS, HEADS * DN)
    value_flat = value_grad.transpose(1, 0, 2).reshape(TOKENS, HEADS * DV)
    rope_grad = lax.optimization_barrier(jnp.sum(key_grad[:, :, DN:], axis=0))
    highest = lax.Precision.HIGHEST
    latent_grad = jnp.dot(key_nope, w_uk.astype(jnp.float32).T, precision=highest) + jnp.dot(value_flat, w_uv.astype(jnp.float32).T, precision=highest)
    latent_f = latent.astype(jnp.float32).T
    weight_uk = jnp.dot(latent_f, key_nope, precision=highest)
    weight_uv = jnp.dot(latent_f, value_flat, precision=highest)
    return (query_out, latent_grad, rope_grad, weight_uk, weight_uv)

def reference(latent, rope, query, grad_out, attn_out, lse, positions, w_uk, w_uv):

    def one_sequence(totals, item):
        seq_latent, seq_rope, seq_query, seq_grads, seq_outputs, seq_lse, seq_order = item
        query_out, latent_grad, rope_grad, weight_uk, weight_uv = sequence_grads(seq_latent, seq_rope, seq_query, seq_grads, seq_outputs, seq_lse, seq_order, w_uk, w_uv)
        return ((totals[0] + weight_uk, totals[1] + weight_uv), (query_out, latent_grad, rope_grad))
    initial = (jnp.zeros((DL, HEADS * DN), jnp.float32), jnp.zeros((DL, HEADS * DV), jnp.float32))
    totals, stacked = lax.scan(one_sequence, initial, (latent, rope, query, grad_out, attn_out, lse, positions))
    return (stacked[0], stacked[1], stacked[2], totals[0].astype(jnp.bfloat16), totals[1].astype(jnp.bfloat16))
```

```python
import math

import jax
import jax.numpy as jnp
from jax import lax
from jax.experimental import pallas as pl
from jax.experimental.pallas import tpu as pltpu
from jax.sharding import PartitionSpec as P

DL = 512
DR = 64
DN = 128
DV = 128
HPD = 4
ROWS = 128
NY = 8
NX = 8
NZ = 4
SL = ROWS // NX
GW = 640
MASKED = -1e30
SCALE = 1.0 / math.sqrt(DN + DR)
MESH = pl.DeviceIdType.MESH
F32 = jnp.float32
BF16 = jnp.bfloat16

OFFS = (0, -1, 1, -2, 2, -3, 3, 4)
GROUPS = ((0, 1), (1, 3), (3, 5), (5, 7), (7, 8))


def wrap(v, n):
    return lax.rem(v + 2 * n, n)


def dot(a, b, ca, cb):
    return lax.dot_general(a, b, (((ca,), (cb,)), ((), ())), preferred_element_type=F32)


def kernel(
    lat_ref, rope_ref, q_ref, go_ref, ao_ref, lse_ref, pos_ref, wuk_ref, wuv_ref,
    dq_out, gl_out, gr_out, guk_out, guv_out,
    lat_all, rope_all, qh, gh, delta, dq_acc, dkv_all, glb, xl, xr,
    ysend, yrecv, zs, zr, axr,
    wgb, wgc, wa, wb, wa_in, wb_in, wa2, wb2, wa2_in, wb2_in,
    ag_s, ag_r, xl_s, xl_r, xr_s, xr_r, y_s, y_r, z_sem, ax_s, ax_r,
    c_s, c_r, wy_s, wy_r, wz_s, wz_r, wy2_s, wy2_r, wz2_s, wz2_r,
):
    dp = lax.axis_index("dp")
    y = lax.axis_index("ctx")
    head = lax.axis_index("head")
    c, zl = lax.rem(dp, 2), dp // 2
    x, zh = head // 2, lax.rem(head, 2)

    def to_y(v):
        return {"ctx": wrap(v, NY)}

    def to_x(v):
        return {"head": wrap(v, NX) * 2 + zh}

    def to_z(v):
        return {"dp": wrap(v, NZ) * 2 + c}

    other_core = {"dp": zl * 2 + (1 - c)}
    other_half = {"head": x * 2 + (1 - zh)}

    barrier = pltpu.get_barrier_semaphore()
    peers = [to_y(y + 1), to_y(y - 1), to_x(x + 1), to_x(x - 1)]
    peers += [to_z(zl + d) for d in range(1, NZ)] + [other_core, other_half]
    for peer in peers:
        pl.semaphore_signal(barrier, inc=1, device_id=peer, device_id_type=MESH)

    started = []

    def send(src, dst, s_sem, r_sem, device):
        copy = pltpu.make_async_remote_copy(
            src_ref=src, dst_ref=dst, send_sem=s_sem, recv_sem=r_sem,
            device_id=device, device_id_type=MESH,
        )
        copy.start()
        started.append(copy)
        return copy

    lat_all[y] = lat_ref[0]
    rope_all[y] = jnp.concatenate([rope_ref[0, 0:64, :], rope_ref[0, 64:128, :]], axis=1)
    for h in range(HPD):
        qh[h] = q_ref[0, :, 192 * h : 192 * h + 192]
        g = go_ref[0, :, 128 * h : 128 * h + 128]
        gh[h] = g
        prod = g.astype(F32) * ao_ref[0, :, 128 * h : 128 * h + 128].astype(F32)
        delta[h : h + 1, :] = jnp.sum(prod.T, axis=0, keepdims=True)

    pl.semaphore_wait(barrier, len(peers))

    def ag_parts(block):
        return (
            lat_all.at[block, pl.ds(0, 64)],
            lat_all.at[block, pl.ds(64, 64)],
            rope_all.at[block],
        )

    ag = {}

    def ag_step(k):
        for part in range(3):
            for way, sign in ((0, 1), (1, -1)):
                if k == 3 and (part == 0) != (way == 0):
                    continue
                if k > 0:
                    ag[way, k - 1, part].wait_recv()
                ref = ag_parts(wrap(y - sign * k, NY))[part]
                ag[way, k, part] = send(
                    ref, ref, ag_s.at[way, k, part], ag_r.at[way, k, part], to_y(y + sign)
                )

    def ag_rest(k):
        for part in range(3):
            for way in (0, 1):
                if k == 3 and (part == 0) != (way == 0):
                    ag[way, k - 1, part].wait_recv()

    pos_q = pos_ref[:, pl.ds(pl.multiple_of(y * ROWS, ROWS), ROWS)].astype(F32)

    def compute(group):
        lo, hi = GROUPS[group]
        blocks = [wrap(y + OFFS[r], NY) for r in range(lo, hi)]
        n = len(blocks)

        def joined(parts):
            return parts[0] if n == 1 else jnp.concatenate(parts, axis=0)

        lat = joined([lat_all[b] for b in blocks])
        ropes, masks = [], []
        for b in blocks:
            packed = rope_all[b]
            ropes += [packed[:, 0:64], packed[:, 64:128]]
            pos_k = pos_ref[:, pl.ds(pl.multiple_of(b * ROWS, ROWS), ROWS)].astype(F32)
            masks.append(jnp.broadcast_to(pos_k, (ROWS, ROWS)).T)
        rope = jnp.concatenate(ropes, axis=0)
        allowed = joined(masks) <= pos_q
        keys = dot(lat, wuk_ref[...], 1, 0).astype(BF16)
        values = dot(lat, wuv_ref[...], 1, 0).astype(BF16)
        rope_grad = None
        dks, dvs = [], []
        for h in range(HPD):
            kh = jnp.concatenate([keys[:, 128 * h : 128 * h + 128], rope], axis=1)
            vh = values[:, 128 * h : 128 * h + 128]
            q, g = qh[h], gh[h]
            scores = dot(kh, q, 1, 1) * SCALE
            dots = dot(vh, g, 1, 1)
            w = jnp.exp(jnp.where(allowed, scores - lse_ref[0, h : h + 1, :], MASKED))
            sg = (w * (dots - delta[h : h + 1, :]) * SCALE).astype(BF16)
            dk = dot(sg, q, 1, 0)
            dv = dot(w.astype(BF16), g, 1, 0)
            dq = dot(sg, kh, 0, 0)
            if group == 0:
                dq_acc[h] = dq
            else:
                dq_acc[h] += dq
            part = dk[:, 128:192]
            rope_grad = part if rope_grad is None else rope_grad + part
            dks.append(dk[:, 0:128].astype(BF16))
            dvs.append(dv.astype(BF16))
        dkn = jnp.concatenate(dks, axis=1)
        dvn = jnp.concatenate(dvs, axis=1)
        for i, b in enumerate(blocks):
            dkv_all[b, :, 0:512] = dkn[128 * i : 128 * i + 128]
            dkv_all[b, :, 512:1024] = dvn[128 * i : 128 * i + 128]
        gl = dot(dkn, wuk_ref[...], 1, 1) + dot(dvn, wuv_ref[...], 1, 1)
        whole = jnp.concatenate([gl, rope_grad, jnp.zeros_like(rope_grad)], axis=1).astype(BF16)
        for i in range(n):
            for s in range(NX):
                at = 128 * i + SL * s
                glb[s, lo + i] = whole[at : at + SL]

    arms = {}

    def hops(group, way):
        return 4 if (group + way) % 2 == 0 else 3

    def chain(group, k):
        lo, hi = GROUPS[group]
        for way, sign, slots, s_sem, r_sem in (
            (0, -1, xl, xl_s, xl_r),
            (1, 1, xr, xr_s, xr_r),
        ):
            length = hops(group, way)
            if k >= length:
                continue
            dest = wrap(x + sign * (length - k), NX)
            own = glb.at[dest, lo:hi]
            src = own
            if k > 0:
                arms[group, way, k - 1].wait_recv()
                src = slots.at[k - 1, lo:hi]
                src[...] = (src[...].astype(F32) + own[...].astype(F32)).astype(BF16)
            arms[group, way, k] = send(
                src, slots.at[k, lo:hi], s_sem.at[group, k], r_sem.at[group, k], to_x(x + sign)
            )

    y_copies = {}

    def chain_end(group):
        lo, hi = GROUPS[group]
        last = (hops(group, 0) - 1, hops(group, 1) - 1)
        for way in (0, 1):
            arms[group, way, last[way]].wait_recv()
        total = (
            glb[x, lo:hi].astype(F32)
            + xl[last[0], lo:hi].astype(F32)
            + xr[last[1], lo:hi].astype(F32)
        )
        ysend[lo:hi] = total.astype(BF16)
        for r in range(lo, hi):
            if r > 0:
                y_copies[r] = send(
                    ysend.at[r], yrecv.at[r], y_s.at[r], y_r.at[r], to_y(y + OFFS[r])
                )

    core_copies = {}

    def weight_rows(z):
        lat = lat_all[:, :, 128 * z : 128 * z + 128].reshape(NY * ROWS, 128)
        rows = dot(lat, dkv_all[...].reshape(NY * ROWS, 1024), 0, 0)
        for half in range(2):
            wgb[half, z] = rows[64 * half : 64 * half + 64].reshape(NY, 8, 1024).astype(BF16)
        core_copies[z] = send(wgb.at[1 - c, z], wgc.at[z], c_s.at[z], c_r.at[z], other_core)

    ag_step(0)
    compute(0)
    chain(0, 0)
    ag_step(1)
    compute(1)
    chain(1, 0)
    chain(0, 1)
    ag_step(2)
    compute(2)
    chain(2, 0)
    chain(1, 1)
    chain(0, 2)
    ag_step(3)
    ag_rest(3)
    compute(3)
    chain(3, 0)
    chain(2, 1)
    chain(1, 2)
    chain(0, 3)
    ag[0, 3, 0].wait_recv()
    ag[1, 3, 1].wait_recv()
    ag[1, 3, 2].wait_recv()
    compute(4)
    chain(4, 0)
    chain(3, 1)
    chain(2, 2)
    chain(1, 3)
    chain_end(0)
    weight_rows(0)
    weight_rows(1)
    chain(4, 1)
    chain(3, 2)
    chain(2, 3)
    chain_end(1)
    weight_rows(2)
    weight_rows(3)
    chain(4, 2)
    chain(3, 3)
    chain_end(2)

    for z in range(NZ):
        core_copies[z].wait_recv()
        both = wgb[c, z].astype(F32) + wgc[z].astype(F32)
        both = both.astype(BF16)
        wa[:, z] = both[:, :, 0:512]
        wb[z] = both[:, :, 512:1024]
    wa_copies, wb_copies = [], []
    for d in (4, 3, 5, 2, 6, 1, 7):
        at = wrap(y + d, NY)
        wa_copies.append(
            send(wa.at[at], wa_in.at[d], wy_s.at[d], wy_r.at[d], to_y(y + d))
        )
    for d in (2, 1, 3):
        at = wrap(zl + d, NZ)
        wb_copies.append(
            send(wb.at[at], wb_in.at[d], wz_s.at[d], wz_r.at[d], to_z(zl + d))
        )
    chain(4, 3)
    chain_end(3)
    chain_end(4)

    for r in range(1, NY):
        y_copies[r].wait_recv()
    total = ysend[0].astype(F32)
    for r in range(1, NY):
        total += yrecv[r].astype(F32)
    zs[...] = total.astype(BF16)
    z_copy = send(zs, zr, z_sem.at[0], z_sem.at[1], other_half)

    for h in range(HPD):
        dq_out[0, :, 192 * h : 192 * h + 192] = dq_acc[h].astype(BF16)

    for copy in wb_copies:
        copy.wait_recv()
    total = wb[zl].astype(F32)
    for d in range(1, NZ):
        total += wb_in[d].astype(F32)
    wb2[...] = total.astype(BF16)
    wb2_copies = []
    for d in (4, 3, 5, 2, 6, 1, 7):
        at = wrap(y + d, NY)
        wb2_copies.append(
            send(wb2.at[at], wb2_in.at[d], wy2_s.at[d], wy2_r.at[d], to_y(y + d))
        )
    z_copy.wait_recv()
    axr[x] = (zs[...].astype(F32) + zr[...].astype(F32)).astype(BF16)
    ax_copies = []
    for d in (4, 3, 5, 2, 6, 1, 7):
        ax_copies.append(
            send(axr.at[x], axr.at[x], ax_s.at[d], ax_r.at[d], to_x(x + d))
        )
    for copy in wa_copies:
        copy.wait_recv()
    total = wa[y].astype(F32)
    for d in range(1, NY):
        total += wa_in[d].astype(F32)
    wa2[...] = total.astype(BF16)
    wa2_copies = []
    for d in (2, 1, 3):
        at = wrap(zl + d, NZ)
        wa2_copies.append(
            send(wa2.at[at], wa2_in.at[d], wz2_s.at[d], wz2_r.at[d], to_z(zl + d))
        )
    for copy in wb2_copies:
        copy.wait_recv()
    total = wb2[y].astype(F32)
    for d in range(1, NY):
        total += wb2_in[d].astype(F32)
    guv_out[...] = total.astype(BF16)
    for copy in wa2_copies:
        copy.wait_recv()
    total = wa2[zl].astype(F32)
    for d in range(1, NZ):
        total += wa2_in[d].astype(F32)
    guk_out[...] = total.astype(BF16)
    for copy in ax_copies:
        copy.wait_recv()
    for s in range(NX):
        gl_out[0, SL * s : SL * s + SL, :] = axr[s, :, 0:512].astype(F32)
        gr_out[0, SL * s : SL * s + SL, :] = axr[s, :, 512:576].astype(F32)
    for copy in started:
        copy.wait_send()


def on_device(latent, rope, query, grad_out, attn_out, lse, positions, w_uk, w_uv):
    vmem = pl.BlockSpec(memory_space=pltpu.VMEM)
    dma = pltpu.SemaphoreType.DMA
    shapes = [
        pltpu.VMEM((NY, ROWS, DL), BF16),
        pltpu.VMEM((NY, 64, 128), BF16),
        pltpu.VMEM((HPD, ROWS, 192), BF16),
        pltpu.VMEM((HPD, ROWS, DV), BF16),
        pltpu.VMEM((8, ROWS), F32),
        pltpu.VMEM((HPD, ROWS, 192), F32),
        pltpu.VMEM((NY, ROWS, 1024), BF16),
        pltpu.VMEM((NX, NY, SL, GW), BF16),
        pltpu.VMEM((4, NY, SL, GW), BF16),
        pltpu.VMEM((4, NY, SL, GW), BF16),
        pltpu.VMEM((NY, SL, GW), BF16),
        pltpu.VMEM((NY, SL, GW), BF16),
        pltpu.VMEM((SL, GW), BF16),
        pltpu.VMEM((SL, GW), BF16),
        pltpu.VMEM((NX, SL, GW), BF16),
        pltpu.VMEM((2, NZ, NY, 8, 1024), BF16),
        pltpu.VMEM((NZ, NY, 8, 1024), BF16),
        pltpu.VMEM((NY, NZ, 8, 512), BF16),
        pltpu.VMEM((NZ, NY, 8, 512), BF16),
        pltpu.VMEM((NY, NZ, 8, 512), BF16),
        pltpu.VMEM((NZ, NY, 8, 512), BF16),
        pltpu.VMEM((NZ, 8, 512), BF16),
        pltpu.VMEM((NY, 8, 512), BF16),
        pltpu.VMEM((NZ, 8, 512), BF16),
        pltpu.VMEM((NY, 8, 512), BF16),
        dma((2, 4, 3)), dma((2, 4, 3)),
        dma((5, 4)), dma((5, 4)), dma((5, 4)), dma((5, 4)),
        dma((NY,)), dma((NY,)), dma((2,)), dma((NX,)), dma((NX,)),
        dma((NZ,)), dma((NZ,)),
        dma((NY,)), dma((NY,)), dma((NZ,)), dma((NZ,)),
        dma((NY,)), dma((NY,)), dma((NZ,)), dma((NZ,)),
    ]
    return pl.pallas_call(
        kernel,
        out_shape=(
            jax.ShapeDtypeStruct((1, ROWS, HPD * 192), BF16),
            jax.ShapeDtypeStruct((1, ROWS, DL), F32),
            jax.ShapeDtypeStruct((1, ROWS, DR), F32),
            jax.ShapeDtypeStruct((8, 512), BF16),
            jax.ShapeDtypeStruct((8, 512), BF16),
        ),
        in_specs=[vmem] * 9,
        out_specs=(vmem,) * 5,
        scratch_shapes=shapes,
        compiler_params=pltpu.CompilerParams(
            collective_id=0, has_side_effects=True, vmem_limit_bytes=60 * 1024 * 1024
        ),
    )(latent, rope, query, grad_out, attn_out, lse, positions, w_uk, w_uv)


def solution(mesh):
    return jax.shard_map(
        on_device,
        mesh=mesh,
        in_specs=(
            P("dp", "ctx", None),
            P("dp", "ctx", None),
            P("dp", "ctx", "head"),
            P("dp", "ctx", "head"),
            P("dp", "ctx", "head"),
            P("dp", "head", "ctx"),
            P("dp", None),
            P(None, "head"),
            P(None, "head"),
        ),
        out_specs=(
            P("dp", "ctx", "head"),
            P("dp", "ctx", None),
            P("dp", "ctx", None),
            P(("dp", "ctx"), "head"),
            P(("dp", "ctx"), "head"),
        ),
        check_vma=False,
    )
```

```python
import math

import jax
import jax.numpy as jnp
from jax import lax
from jax.experimental import pallas as pl
from jax.experimental.pallas import tpu as pltpu
from jax.sharding import PartitionSpec as P

DL = 512
DR = 64
DN = 128
DV = 128
HPD = 4
ROWS = 128
NY = 8
NX = 8
NZ = 4
SL = ROWS // NX
GR = 72
QR = 144
MASKED = -1e30
SCALE = 1.0 / math.sqrt(DN + DR)
VMEM_LIMIT = 40 * 1024 * 1024
MESH = pl.DeviceIdType.MESH
F32 = jnp.float32
BF16 = jnp.bfloat16

OFFS = (0, -1, 1, -2, 2, -3, 3, 4)
GROUPS = ((0, 1), (1, 3), (3, 5), (5, 7), (7, 8))


def wrap(v, n):
    return lax.rem(v + 2 * n, n)


def dot(a, b, ca, cb):
    return lax.dot_general(a, b, (((ca,), (cb,)), ((), ())), preferred_element_type=F32)


def kernel(
    lat_hbm, rope_hbm, lse_hbm, pos_hbm, q_hbm, go_hbm, ao_hbm, wuk_hbm, wuv_hbm,
    dq_out, ax_out, guk_out, guv_out,
    lat_ref, rope_ref, lse_ref, pos_ref, q_ref, go_ref, ao_ref, wuk_ref, wuv_ref,
    kv_all, qh, gh, delta, dq_acc, dkv_all, glb, xl, xr, ysend, yrecv, zs, zr, axr,
    wgb, wgc, wa, wb, wa_in, wb_in, wa2, wb2, wa2_in, wb2_in,
    in_sem, ag_s, ag_r, agx_s, agx_r, xl_s, xl_r, xr_s, xr_r, y_sem, z_sem, ax_sem,
    c_sem, wy_sem, wz_sem, wy2_sem, wz2_sem,
):
    dp = lax.axis_index("dp")
    y = lax.axis_index("ctx")
    head = lax.axis_index("head")
    c, zl = lax.rem(dp, 2), dp // 2
    x, zh = head // 2, lax.rem(head, 2)
    side = lax.rem(x, 2)

    def to_y(v):
        return {"ctx": wrap(v, NY)}

    def to_x(v):
        return {"head": wrap(v, NX) * 2 + zh}

    def to_z(v):
        return {"dp": wrap(v, NZ) * 2 + c}

    other_core = {"dp": zl * 2 + (1 - c)}
    other_half = {"head": x * 2 + (1 - zh)}

    barrier = pltpu.get_barrier_semaphore()
    peers = [to_y(y + 1), to_y(y - 1), to_x(x + 1), to_x(x - 1)]
    peers += [to_z(zl + d) for d in range(1, NZ)] + [other_core, other_half]
    for peer in peers:
        pl.semaphore_signal(barrier, inc=1, device_id=peer, device_id_type=MESH)

    loads = []
    for i, (a, b) in enumerate(
        (
            (lat_hbm, lat_ref), (rope_hbm, rope_ref), (q_hbm, q_ref), (go_hbm, go_ref),
            (ao_hbm, ao_ref), (lse_hbm, lse_ref), (pos_hbm, pos_ref), (wuk_hbm, wuk_ref),
            (wuv_hbm, wuv_ref),
        )
    ):
        loads.append(pltpu.make_async_copy(a, b, in_sem.at[i]))
        loads[i].start()

    def copy_of(src, dst, s_sem, r_sem, device):
        return pltpu.make_async_remote_copy(
            src_ref=src, dst_ref=dst, send_sem=s_sem, recv_sem=r_sem,
            device_id=device, device_id_type=MESH,
        )

    def send(src, dst, s_sem, r_sem, device):
        copy = copy_of(src, dst, s_sem, r_sem, device)
        copy.start()
        return copy

    loads[0].wait()
    loads[1].wait()
    for t in range(4):
        for ct in range(4):
            kv_all[y, t, 32 * ct : 32 * ct + 32, :] = lat_ref[
                0, 32 * t : 32 * t + 32, 128 * ct : 128 * ct + 128
            ]
        kv_all[y, t, 128:144, :] = rope_ref[0, 16 * t : 16 * t + 16, :]

    pl.semaphore_wait(barrier, len(peers))

    ag, agx = {}, {}

    def ag_step(k):
        for part in range(2):
            for way, sign in ((0, 1), (1, -1)):
                if k == 4 and part != way:
                    continue
                if k > 0:
                    ag[way, k - 1, part].wait_recv()
                ref = kv_all.at[wrap(y - sign * k, NY), 2 * side + part]
                if k < 3 or (k == 3 and part == way):
                    ag[way, k, part] = send(
                        ref, ref, ag_s.at[way], ag_r.at[way, k, part], to_y(y + sign)
                    )
                if k > 0:
                    r = 2 * k - 1 + way if k < 4 else 7
                    agx[r, part] = send(
                        ref, ref, agx_s.at[part], agx_r.at[r, part], to_x(x + 1 - 2 * part)
                    )

    def agx_wait(group):
        for r in range(*GROUPS[group]):
            for part in range(2):
                agx[r, part].wait_recv()

    def prepare():
        for load in loads[2:]:
            load.wait()
        for h in range(HPD):
            qh[h] = q_ref[0, :, 192 * h : 192 * h + 192]
            g = go_ref[0, :, 128 * h : 128 * h + 128]
            gh[h] = g
            prod = g.astype(F32) * ao_ref[0, :, 128 * h : 128 * h + 128].astype(F32)
            delta[h : h + 1, :] = jnp.sum(prod.T, axis=0, keepdims=True)

    def lat_of(b):
        quarters = [
            jnp.concatenate([kv_all[b, t, 32 * ct : 32 * ct + 32, :] for ct in range(4)], axis=1)
            for t in range(4)
        ]
        return jnp.concatenate(quarters, axis=0)

    def rope_of(b):
        return jnp.concatenate([kv_all[b, t, 128:144, :] for t in range(4)], axis=0).T

    def compute(group):
        pos_q = pos_ref[:, pl.ds(pl.multiple_of(y * ROWS, ROWS), ROWS)].astype(F32)
        lo, hi = GROUPS[group]
        blocks = [wrap(y + OFFS[r], NY) for r in range(lo, hi)]
        n = len(blocks)

        def joined(parts):
            return parts[0] if n == 1 else jnp.concatenate(parts, axis=0)

        masks = []
        for b in blocks:
            pos_k = pos_ref[:, pl.ds(pl.multiple_of(b * ROWS, ROWS), ROWS)].astype(F32)
            masks.append(jnp.broadcast_to(pos_k, (ROWS, ROWS)).T)
        lat = joined([lat_of(b) for b in blocks])
        rope = joined([rope_of(b) for b in blocks])
        allowed = joined(masks) <= pos_q
        keys = dot(lat, wuk_ref[...], 1, 0).astype(BF16)
        values = dot(lat, wuv_ref[...], 1, 0).astype(BF16)
        rope_grad = None
        dks, dvs = [], []
        for h in range(HPD):
            kh = jnp.concatenate([keys[:, 128 * h : 128 * h + 128], rope], axis=1)
            vh = values[:, 128 * h : 128 * h + 128]
            q, g = qh[h], gh[h]
            scores = dot(kh, q, 1, 1) * SCALE
            dots = dot(vh, g, 1, 1)
            w = jnp.exp(jnp.where(allowed, scores - lse_ref[0, h : h + 1, :], MASKED))
            sg = (w * (dots - delta[h : h + 1, :]) * SCALE).astype(BF16)
            dk = dot(sg, q, 1, 0)
            dv = dot(w.astype(BF16), g, 1, 0)
            dq = dot(sg, kh, 0, 0)
            if group == 0:
                dq_acc[h] = dq
            else:
                dq_acc[h] += dq
            part = dk[:, 128:192]
            rope_grad = part if rope_grad is None else rope_grad + part
            dks.append(dk[:, 0:128].astype(BF16))
            dvs.append(dv.astype(BF16))
        dkn = jnp.concatenate(dks, axis=1)
        dvn = jnp.concatenate(dvs, axis=1)
        for i, b in enumerate(blocks):
            dkv_all[b, :, 0:512] = dkn[128 * i : 128 * i + 128]
            dkv_all[b, :, 512:1024] = dvn[128 * i : 128 * i + 128]
        gl = (dot(dkn, wuk_ref[...], 1, 1) + dot(dvn, wuv_ref[...], 1, 1)).astype(BF16)
        for i in range(n):
            turned = rope_grad[128 * i : 128 * i + 128].T
            for s in range(NX):
                at = 128 * i + SL * s
                for ct in range(4):
                    glb[s, lo + i, 16 * ct : 16 * ct + 16, :] = gl[
                        at : at + SL, 128 * ct : 128 * ct + 128
                    ]
                glb[s, lo + i, 64:72, :] = turned[8 * s : 8 * s + 8].astype(BF16)

    arms = {}

    def hops(group, way):
        return 4 if (group + way) % 2 == 0 else 3

    def chain(group, k):
        lo, hi = GROUPS[group]
        for way, sign, slots, s_sem, r_sem in (
            (0, -1, xl, xl_s, xl_r),
            (1, 1, xr, xr_s, xr_r),
        ):
            length = hops(group, way)
            if k >= length:
                continue
            dest = wrap(x + sign * (length - k), NX)
            own = glb.at[dest, lo:hi]
            src = own
            if k > 0:
                arms[group, way, k - 1].wait_recv()
                src = slots.at[k - 1, lo:hi]
                src[...] = (src[...].astype(F32) + own[...].astype(F32)).astype(BF16)
            arms[group, way, k] = send(
                src, slots.at[k, lo:hi], s_sem.at[group], r_sem.at[group, k], to_x(x + sign)
            )

    def chain_end(group):
        lo, hi = GROUPS[group]
        last = (hops(group, 0) - 1, hops(group, 1) - 1)
        for way in (0, 1):
            arms[group, way, last[way]].wait_recv()
        total = (
            glb[x, lo:hi].astype(F32)
            + xl[last[0], lo:hi].astype(F32)
            + xr[last[1], lo:hi].astype(F32)
        )
        ysend[lo:hi] = total.astype(BF16)
        for r in range(lo, hi):
            if r > 0:
                send(ysend.at[r], yrecv.at[r], y_sem.at[0], y_sem.at[1], to_y(y + OFFS[r]))

    def weight_rows(z):
        lat = kv_all[:, :, 32 * z : 32 * z + 32, :].reshape(NY * ROWS, 128)
        rows = dot(lat, dkv_all[...].reshape(NY * ROWS, 1024), 0, 0)
        for half in range(2):
            wgb[half, z] = rows[64 * half : 64 * half + 64].reshape(NY, 8, 1024).astype(BF16)
        send(wgb.at[1 - c, z], wgc.at[z], c_sem.at[0], c_sem.at[1], other_core)

    def spread(src, dst, sem, n, me, to):
        order = (4, 3, 5, 2, 6, 1, 7) if n == 8 else (2, 1, 3)
        for d in order:
            send(src.at[wrap(me + d, n)], dst.at[d], sem.at[0], sem.at[1], to(me + d))

    def whole(ref, sem):
        return copy_of(ref, ref, sem.at[0], sem.at[1], other_half)

    def summed(own, got, n):
        total = own.astype(F32)
        for d in range(1, n):
            total += got[d].astype(F32)
        return total.astype(BF16)

    ag_step(0)
    prepare()
    compute(0)
    chain(0, 0)
    ag_step(1)
    ag_step(2)
    chain(0, 1)
    agx_wait(1)
    compute(1)
    chain(1, 0)
    ag_step(3)
    chain(0, 2)
    agx_wait(2)
    compute(2)
    chain(2, 0)
    ag_step(4)
    chain(1, 1)
    chain(0, 3)
    agx_wait(3)
    compute(3)
    chain(3, 0)
    chain(2, 1)
    chain(1, 2)
    agx_wait(4)
    compute(4)
    chain(4, 0)
    chain(3, 1)
    chain(2, 2)
    chain(1, 3)
    chain_end(0)
    weight_rows(0)
    weight_rows(1)
    chain(4, 1)
    chain(3, 2)
    chain(2, 3)
    chain_end(1)
    weight_rows(2)
    weight_rows(3)
    chain(4, 2)
    chain(3, 3)
    chain_end(2)
    for h in range(HPD):
        dq_out[0, :, 192 * h : 192 * h + 192] = dq_acc[h].astype(BF16)
    chain(4, 3)
    chain_end(3)
    chain_end(4)

    whole(wgc, c_sem).wait_recv()
    for z in range(NZ):
        both = (wgb[c, z].astype(F32) + wgc[z].astype(F32)).astype(BF16)
        wa[:, z] = both[:, :, 0:512]
        wb[z] = both[:, :, 512:1024]
    spread(wb, wb_in, wz_sem, NZ, zl, to_z)
    spread(wa, wa_in, wy_sem, NY, y, to_y)

    whole(yrecv.at[1:8], y_sem).wait_recv()
    zs[...] = summed(ysend[0], yrecv, NY)
    z_copy = send(zs, zr, z_sem.at[0], z_sem.at[1], other_half)

    whole(wb_in.at[1:4], wz_sem).wait_recv()
    wb2[...] = summed(wb[zl], wb_in, NZ)
    spread(wb2, wb2_in, wy2_sem, NY, y, to_y)

    z_copy.wait_recv()
    axr[x] = (zs[...].astype(F32) + zr[...].astype(F32)).astype(BF16)
    for d in (4, 3, 5, 2, 6, 1, 7):
        send(axr.at[x], axr.at[x], ax_sem.at[0], ax_sem.at[1], to_x(x + d))

    whole(wa_in.at[1:8], wy_sem).wait_recv()
    wa2[...] = summed(wa[y], wa_in, NY)
    spread(wa2, wa2_in, wz2_sem, NZ, zl, to_z)

    whole(wb2_in.at[1:8], wy2_sem).wait_recv()
    guv_out[...] = summed(wb2[y], wb2_in, NY)
    whole(wa2_in.at[1:4], wz2_sem).wait_recv()
    guk_out[...] = summed(wa2[zl], wa2_in, NZ)
    whole(axr.at[1:8], ax_sem).wait_recv()
    ax_out[...] = axr[...]

    for sem in (ag_s.at[0], ag_s.at[1], agx_s.at[0], agx_s.at[1]):
        copy_of(glb.at[1:8, 0:2], glb.at[1:8, 0:2], sem, sem, other_half).wait_send()
    for way, slots, s_sem in ((0, xl, xl_s), (1, xr, xr_s)):
        for group, (lo, hi) in enumerate(GROUPS):
            part = slots.at[0 : hops(group, way), lo:hi]
            copy_of(part, part, s_sem.at[group], s_sem.at[group], other_half).wait_send()
    for ref, sem in (
        (wgc, c_sem), (yrecv.at[1:8], y_sem), (zr, z_sem), (axr.at[1:8], ax_sem),
        (wb_in.at[1:4], wz_sem), (wa_in.at[1:8], wy_sem),
        (wb2_in.at[1:8], wy2_sem), (wa2_in.at[1:4], wz2_sem),
    ):
        whole(ref, sem).wait_send()


def finish(dq_ref, ax_ref, guk_ref, guv_ref, dq_out, gl_out, gr_out, guk_out, guv_out):
    dq_out[...] = dq_ref[...]
    for s in range(NX):
        for ct in range(4):
            gl_out[0, SL * s : SL * s + SL, 128 * ct : 128 * ct + 128] = ax_ref[
                s, 16 * ct : 16 * ct + 16, :
            ].astype(F32)
        gr_out[0, 8 * s : 8 * s + 8, :] = ax_ref[s, 64:72, :].astype(F32)
    guk_out[...] = guk_ref[...]
    guv_out[...] = guv_ref[...]


def on_device(latent, rope, query, grad_out, attn_out, lse, positions, w_uk, w_uv):
    vmem = pl.BlockSpec(memory_space=pltpu.VMEM)
    hbm = pl.BlockSpec(memory_space=pltpu.HBM)
    dma = pltpu.SemaphoreType.DMA
    shapes = [
        pltpu.VMEM((1, ROWS, DL), BF16),
        pltpu.VMEM((1, DR, ROWS), BF16),
        pltpu.VMEM((1, HPD, ROWS), F32),
        pltpu.VMEM((1, NY * ROWS), jnp.int32),
        pltpu.VMEM((1, ROWS, HPD * 192), BF16),
        pltpu.VMEM((1, ROWS, HPD * DV), BF16),
        pltpu.VMEM((1, ROWS, HPD * DV), BF16),
        pltpu.VMEM((DL, 512), BF16),
        pltpu.VMEM((DL, 512), BF16),
        pltpu.VMEM((NY, 4, QR, 128), BF16),
        pltpu.VMEM((HPD, ROWS, 192), BF16),
        pltpu.VMEM((HPD, ROWS, DV), BF16),
        pltpu.VMEM((8, ROWS), F32),
        pltpu.VMEM((HPD, ROWS, 192), F32),
        pltpu.VMEM((NY, ROWS, 1024), BF16),
        pltpu.VMEM((NX, NY, GR, 128), BF16),
        pltpu.VMEM((4, NY, GR, 128), BF16),
        pltpu.VMEM((4, NY, GR, 128), BF16),
        pltpu.VMEM((NY, GR, 128), BF16),
        pltpu.VMEM((NY, GR, 128), BF16),
        pltpu.VMEM((GR, 128), BF16),
        pltpu.VMEM((GR, 128), BF16),
        pltpu.VMEM((NX, GR, 128), BF16),
        pltpu.VMEM((2, NZ, NY, 8, 1024), BF16),
        pltpu.VMEM((NZ, NY, 8, 1024), BF16),
        pltpu.VMEM((NY, NZ, 8, 512), BF16),
        pltpu.VMEM((NZ, NY, 8, 512), BF16),
        pltpu.VMEM((NY, NZ, 8, 512), BF16),
        pltpu.VMEM((NZ, NY, 8, 512), BF16),
        pltpu.VMEM((NZ, 8, 512), BF16),
        pltpu.VMEM((NY, 8, 512), BF16),
        pltpu.VMEM((NZ, 8, 512), BF16),
        pltpu.VMEM((NY, 8, 512), BF16),
        dma((9,)),
        dma((2,)), dma((2, 4, 2)), dma((2,)), dma((NY, 2)),
        dma((5,)), dma((5, 4)), dma((5,)), dma((5, 4)),
        dma((2,)), dma((2,)), dma((2,)),
        dma((2,)), dma((2,)), dma((2,)), dma((2,)), dma((2,)),
    ]
    dq, ax, guk, guv = pl.pallas_call(
        kernel,
        out_shape=(
            jax.ShapeDtypeStruct((1, ROWS, HPD * 192), BF16),
            jax.ShapeDtypeStruct((NX, GR, 128), BF16),
            jax.ShapeDtypeStruct((8, 512), BF16),
            jax.ShapeDtypeStruct((8, 512), BF16),
        ),
        in_specs=[hbm] * 9,
        out_specs=(vmem,) * 4,
        scratch_shapes=shapes,
        compiler_params=pltpu.CompilerParams(
            collective_id=0, has_side_effects=True, vmem_limit_bytes=VMEM_LIMIT
        ),
    )(
        *(
            pltpu.with_memory_space_constraint(a, pltpu.HBM)
            for a in (
                latent, jnp.transpose(rope, (0, 2, 1)), lse, positions,
                query, grad_out, attn_out, w_uk, w_uv,
            )
        )
    )
    dq, gl, gr, guk, guv = pl.pallas_call(
        finish,
        out_shape=(
            jax.ShapeDtypeStruct((1, ROWS, HPD * 192), BF16),
            jax.ShapeDtypeStruct((1, ROWS, DL), F32),
            jax.ShapeDtypeStruct((1, DR, ROWS), F32),
            jax.ShapeDtypeStruct((8, 512), BF16),
            jax.ShapeDtypeStruct((8, 512), BF16),
        ),
        in_specs=[vmem] * 4,
        out_specs=(vmem,) * 5,
        compiler_params=pltpu.CompilerParams(vmem_limit_bytes=8 * 1024 * 1024),
    )(dq, ax, guk, guv)
    return dq, gl, jnp.transpose(gr, (0, 2, 1)), guk, guv


def solution(mesh):
    return jax.shard_map(
        on_device,
        mesh=mesh,
        in_specs=(
            P("dp", "ctx", None),
            P("dp", "ctx", None),
            P("dp", "ctx", "head"),
            P("dp", "ctx", "head"),
            P("dp", "ctx", "head"),
            P("dp", "head", "ctx"),
            P("dp", None),
            P(None, "head"),
            P(None, "head"),
        ),
        out_specs=(
            P("dp", "ctx", "head"),
            P("dp", "ctx", None),
            P("dp", "ctx", None),
            P(("dp", "ctx"), "head"),
            P(("dp", "ctx"), "head"),
        ),
        check_vma=False,
    )
```

```python
import math

import jax
import jax.numpy as jnp
from jax import lax
from jax.experimental import pallas as pl
from jax.experimental.pallas import tpu as pltpu
from jax.sharding import PartitionSpec as P

DL = 512
DR = 64
DN = 128
DV = 128
HPD = 4
ROWS = 128
NY = 8
NX = 8
NZ = 4
SL = ROWS // NX
GR = 72
QR = 144
MASKED = -1e30
SCALE = 1.0 / math.sqrt(DN + DR)
VMEM_LIMIT = 40 * 1024 * 1024
MESH = pl.DeviceIdType.MESH
F32 = jnp.float32
BF16 = jnp.bfloat16

OFFS = (0, -1, 1, -2, 2, -3, 3, 4)
GROUPS = ((0, 1), (1, 3), (3, 5), (5, 7), (7, 8))


def wrap(v, n):
    return lax.rem(v + 2 * n, n)


def dot(a, b, ca, cb):
    return lax.dot_general(a, b, (((ca,), (cb,)), ((), ())), preferred_element_type=F32)


def kernel(
    lat_hbm, rope_hbm, lse_hbm, pos_hbm, q_hbm, go_hbm, ao_hbm, wuk_hbm, wuv_hbm,
    dq_out, ax_out, guk_out, guv_out,
    lat_ref, rope_ref, lse_ref, pos_ref, q_ref, go_ref, ao_ref, wuk_ref, wuv_ref,
    kv_all, qh, gh, delta, dq_acc, dkv_all, glb, xb, ysend, yrecv, zs, zr, axr,
    wgb, wgc, wa, wb, wa_in, wb_in, wa2, wb2, wa2_in, wb2_in,
    in_sem, ag_s, ag_r, x_s, x_r, y_sem, z_sem, ax_sem,
    c_sem, wy_sem, wz_sem, wy2_sem, wz2_sem, up_sem, down_sem,
):
    dp = lax.axis_index("dp")
    y = lax.axis_index("ctx")
    head = lax.axis_index("head")
    c, zl = lax.rem(dp, 2), dp // 2
    x, zh = head // 2, lax.rem(head, 2)
    z = zh * NZ + zl

    def to_y(v):
        return {"ctx": wrap(v, NY)}

    def to_x(v):
        return {"head": wrap(v, NX) * 2 + zh}

    def to_z(v):
        return {"dp": wrap(v, NZ) * 2 + c}

    other_core = {"dp": zl * 2 + (1 - c)}
    other_half = {"head": x * 2 + (1 - zh)}

    def on_line(v):
        return {"dp": lax.rem(v, NZ) * 2 + c, "head": x * 2 + v // NZ}

    def tell(sem, peer):
        pl.semaphore_signal(sem, inc=1, device_id=peer, device_id_type=MESH)

    barrier = pltpu.get_barrier_semaphore()
    peers = [to_y(y + 1), to_y(y - 1), to_x(x + 1), to_x(x - 1), to_x(x + 2), to_x(x - 2)]
    peers.append(other_core)
    for peer in peers:
        tell(barrier, peer)

    @pl.when(z > 0)
    def _():
        tell(barrier, on_line(z - 1))

    @pl.when(z < 7)
    def _():
        tell(barrier, on_line(z + 1))

    def pass_word(j):
        @pl.when((z >= 1) & (z + j <= 7))
        def _():
            tell(up_sem.at[j - 1], on_line(z - 1))

        @pl.when((z <= 6) & (z - j >= 0))
        def _():
            tell(down_sem.at[j - 1], on_line(z + 1))

    def take_word(j):
        @pl.when(z + j <= 6)
        def _():
            pl.semaphore_wait(up_sem.at[j - 1], 1)

        @pl.when(z - j >= 1)
        def _():
            pl.semaphore_wait(down_sem.at[j - 1], 1)

    loads = []
    for i, (a, b) in enumerate(
        (
            (lat_hbm, lat_ref), (rope_hbm, rope_ref), (q_hbm, q_ref), (go_hbm, go_ref),
            (ao_hbm, ao_ref), (lse_hbm, lse_ref), (pos_hbm, pos_ref), (wuk_hbm, wuk_ref),
            (wuv_hbm, wuv_ref),
        )
    ):
        loads.append(pltpu.make_async_copy(a, b, in_sem.at[i]))
        loads[i].start()

    def copy_of(src, dst, s_sem, r_sem, device):
        return pltpu.make_async_remote_copy(
            src_ref=src, dst_ref=dst, send_sem=s_sem, recv_sem=r_sem,
            device_id=device, device_id_type=MESH,
        )

    def send(src, dst, s_sem, r_sem, device):
        copy = copy_of(src, dst, s_sem, r_sem, device)
        copy.start()
        return copy

    loads[0].wait()
    loads[1].wait()
    for t in range(4):
        for ct in range(4):
            kv_all[y, t, 32 * ct : 32 * ct + 32, :] = lat_ref[
                0, 32 * t : 32 * t + 32, 128 * ct : 128 * ct + 128
            ]
        kv_all[y, t, 128:144, :] = rope_ref[0, 16 * t : 16 * t + 16, :]

    pl.semaphore_wait(barrier, len(peers) + jnp.minimum(z, 1) + jnp.minimum(7 - z, 1))

    ag = {}

    def ag_step(k, pieces=range(4)):
        for part in pieces:
            for way, sign in ((0, 1), (1, -1)):
                last = part // 2 == way
                if k == 4 and not last:
                    continue
                if k > 0:
                    ag[way, k - 1, part].wait_recv()
                if k < 3 or (k == 3 and last):
                    ref = kv_all.at[wrap(y - sign * k, NY), part]
                    ag[way, k, part] = send(
                        ref, ref, ag_s.at[way], ag_r.at[way, k, part], to_y(y + sign)
                    )

    def prepare():
        for load in loads[2:]:
            load.wait()
        for h in range(HPD):
            qh[h] = q_ref[0, :, 192 * h : 192 * h + 192]
            g = go_ref[0, :, 128 * h : 128 * h + 128]
            gh[h] = g
            prod = g.astype(F32) * ao_ref[0, :, 128 * h : 128 * h + 128].astype(F32)
            delta[h : h + 1, :] = jnp.sum(prod.T, axis=0, keepdims=True)

    def lat_of(b):
        quarters = [
            jnp.concatenate([kv_all[b, t, 32 * ct : 32 * ct + 32, :] for ct in range(4)], axis=1)
            for t in range(4)
        ]
        return jnp.concatenate(quarters, axis=0)

    def rope_of(b):
        return jnp.concatenate([kv_all[b, t, 128:144, :] for t in range(4)], axis=0).T

    def compute(group, between=None):
        pos_q = pos_ref[:, pl.ds(pl.multiple_of(y * ROWS, ROWS), ROWS)].astype(F32)
        lo, hi = GROUPS[group]
        blocks = [wrap(y + OFFS[r], NY) for r in range(lo, hi)]
        n = len(blocks)

        def joined(parts):
            return parts[0] if n == 1 else jnp.concatenate(parts, axis=0)

        masks = []
        for b in blocks:
            pos_k = pos_ref[:, pl.ds(pl.multiple_of(b * ROWS, ROWS), ROWS)].astype(F32)
            masks.append(jnp.broadcast_to(pos_k, (ROWS, ROWS)).T)
        lat = joined([lat_of(b) for b in blocks])
        rope = joined([rope_of(b) for b in blocks])
        allowed = joined(masks) <= pos_q
        keys = dot(lat, wuk_ref[...], 1, 0).astype(BF16)
        values = dot(lat, wuv_ref[...], 1, 0).astype(BF16)
        rope_grad = None
        dks, dvs = [], []
        for h in range(HPD):
            kh = jnp.concatenate([keys[:, 128 * h : 128 * h + 128], rope], axis=1)
            vh = values[:, 128 * h : 128 * h + 128]
            q, g = qh[h], gh[h]
            scores = dot(kh, q, 1, 1) * SCALE
            dots = dot(vh, g, 1, 1)
            w = jnp.exp(jnp.where(allowed, scores - lse_ref[0, h : h + 1, :], MASKED))
            sg = (w * (dots - delta[h : h + 1, :]) * SCALE).astype(BF16)
            dk = dot(sg, q, 1, 0)
            dv = dot(w.astype(BF16), g, 1, 0)
            dq = dot(sg, kh, 0, 0)
            if group == 0:
                dq_acc[h] = dq
            else:
                dq_acc[h] += dq
            part = dk[:, 128:192]
            rope_grad = part if rope_grad is None else rope_grad + part
            dks.append(dk[:, 0:128].astype(BF16))
            dvs.append(dv.astype(BF16))
            if between is not None and h == 1:
                between()
        dkn = jnp.concatenate(dks, axis=1)
        dvn = jnp.concatenate(dvs, axis=1)
        for i, b in enumerate(blocks):
            dkv_all[b, :, 0:512] = dkn[128 * i : 128 * i + 128]
            dkv_all[b, :, 512:1024] = dvn[128 * i : 128 * i + 128]
        gl = (dot(dkn, wuk_ref[...], 1, 1) + dot(dvn, wuv_ref[...], 1, 1)).astype(BF16)
        for i in range(n):
            turned = rope_grad[128 * i : 128 * i + 128].T
            for s in range(NX):
                at = 128 * i + SL * s
                for ct in range(4):
                    glb[s, lo + i, 16 * ct : 16 * ct + 16, :] = gl[
                        at : at + SL, 128 * ct : 128 * ct + 128
                    ]
                glb[s, lo + i, 64:72, :] = turned[8 * s : 8 * s + 8].astype(BF16)

    sums = {}

    def x_send(group, slot, src, step):
        lo, hi = GROUPS[group]
        sums[group, slot] = send(
            src, xb.at[slot, lo:hi], x_s.at[slot], x_r.at[group, slot], to_x(x + step)
        )

    def x_start(group):
        lo, hi = GROUPS[group]
        g = 1 - 2 * (group % 2)
        for slot, dest, step in (
            (0, -4 * g, -2 * g), (1, -3 * g, -g), (2, 3 * g, g), (3, -g, -g), (4, g, g),
        ):
            x_send(group, slot, glb.at[wrap(x + dest, NX), lo:hi], step)

    def x_middle(group):
        lo, hi = GROUPS[group]
        g = 1 - 2 * (group % 2)
        sums[group, 0].wait_recv()
        sums[group, 1].wait_recv()
        xb[0, lo:hi] = (
            xb[0, lo:hi].astype(F32)
            + xb[1, lo:hi].astype(F32)
            + glb[wrap(x - 2 * g, NX), lo:hi].astype(F32)
        ).astype(BF16)
        x_send(group, 5, xb.at[0, lo:hi], -2 * g)
        sums[group, 2].wait_recv()
        xb[2, lo:hi] = (
            xb[2, lo:hi].astype(F32) + glb[wrap(x + 2 * g, NX), lo:hi].astype(F32)
        ).astype(BF16)
        x_send(group, 6, xb.at[2, lo:hi], 2 * g)

    def x_end(group):
        lo, hi = GROUPS[group]
        total = glb[x, lo:hi].astype(F32)
        for slot in (3, 4, 5, 6):
            sums[group, slot].wait_recv()
            total += xb[slot, lo:hi].astype(F32)
        ysend[lo:hi] = total.astype(BF16)
        for r in range(lo, hi):
            if r > 0:
                send(ysend.at[r], yrecv.at[r], y_sem.at[0], y_sem.at[1], to_y(y + OFFS[r]))

    def weight_rows(i):
        lat = kv_all[:, :, 32 * i : 32 * i + 32, :].reshape(NY * ROWS, 128)
        rows = dot(lat, dkv_all[...].reshape(NY * ROWS, 1024), 0, 0)
        for half in range(2):
            wgb[half, i] = rows[64 * half : 64 * half + 64].reshape(NY, 8, 1024).astype(BF16)
        send(wgb.at[1 - c, i], wgc.at[i], c_sem.at[0], c_sem.at[1], other_core)

    def spread(src, dst, sem, n, me, to):
        order = (4, 3, 5, 2, 6, 1, 7) if n == 8 else (2, 1, 3)
        for d in order:
            send(src.at[wrap(me + d, n)], dst.at[d], sem.at[0], sem.at[1], to(me + d))

    def whole(ref, sem):
        return copy_of(ref, ref, sem.at[0], sem.at[1], other_half)

    def summed(own, got, n):
        total = own.astype(F32)
        for d in range(1, n):
            total += got[d].astype(F32)
        return total.astype(BF16)

    ag_step(0)
    pass_word(1)
    prepare()
    compute(0)
    x_start(0)
    ag_step(1)
    compute(1, lambda: ag_step(2, (0,)))
    x_start(1)
    take_word(1)
    pass_word(2)
    ag_step(2, (1, 2, 3))
    x_middle(0)
    compute(2, lambda: ag_step(3, (0,)))
    x_start(2)
    ag_step(3, (1, 2, 3))
    x_middle(1)
    x_end(0)
    compute(3)
    x_start(3)
    take_word(2)
    pass_word(3)
    ag_step(4)
    compute(4)
    x_start(4)
    x_middle(2)
    x_end(1)
    weight_rows(0)
    weight_rows(1)
    x_middle(3)
    x_end(2)
    weight_rows(2)
    weight_rows(3)
    x_middle(4)
    for h in range(HPD):
        dq_out[0, :, 192 * h : 192 * h + 192] = dq_acc[h].astype(BF16)
    take_word(3)
    x_end(3)

    whole(wgc, c_sem).wait_recv()
    for i in range(NZ):
        both = (wgb[c, i].astype(F32) + wgc[i].astype(F32)).astype(BF16)
        wa[:, i] = both[:, :, 0:512]
        wb[i] = both[:, :, 512:1024]
    spread(wb, wb_in, wz_sem, NZ, zl, to_z)
    x_end(4)
    spread(wa, wa_in, wy_sem, NY, y, to_y)

    whole(yrecv.at[1:8], y_sem).wait_recv()
    zs[...] = summed(ysend[0], yrecv, NY)
    z_copy = send(zs, zr, z_sem.at[0], z_sem.at[1], other_half)

    whole(wb_in.at[1:4], wz_sem).wait_recv()
    wb2[...] = summed(wb[zl], wb_in, NZ)
    spread(wb2, wb2_in, wy2_sem, NY, y, to_y)

    z_copy.wait_recv()
    axr[x] = (zs[...].astype(F32) + zr[...].astype(F32)).astype(BF16)
    for d in (4, 3, 5, 2, 6, 1, 7):
        send(axr.at[x], axr.at[x], ax_sem.at[0], ax_sem.at[1], to_x(x + d))

    whole(wa_in.at[1:8], wy_sem).wait_recv()
    wa2[...] = summed(wa[y], wa_in, NY)
    spread(wa2, wa2_in, wz2_sem, NZ, zl, to_z)

    whole(wb2_in.at[1:8], wy2_sem).wait_recv()
    guv_out[...] = summed(wb2[y], wb2_in, NY)
    whole(wa2_in.at[1:4], wz2_sem).wait_recv()
    guk_out[...] = summed(wa2[zl], wa2_in, NZ)
    whole(axr.at[1:8], ax_sem).wait_recv()
    ax_out[...] = axr[...]

    for way in (0, 1):
        copy_of(
            glb.at[1:8, 0:4], glb.at[1:8, 0:4], ag_s.at[way], ag_s.at[way], other_half
        ).wait_send()
    for slot in range(7):
        copy_of(xb.at[slot], xb.at[slot], x_s.at[slot], x_s.at[slot], other_half).wait_send()
    for ref, sem in (
        (wgc, c_sem), (yrecv.at[1:8], y_sem), (zr, z_sem), (axr.at[1:8], ax_sem),
        (wb_in.at[1:4], wz_sem), (wa_in.at[1:8], wy_sem),
        (wb2_in.at[1:8], wy2_sem), (wa2_in.at[1:4], wz2_sem),
    ):
        whole(ref, sem).wait_send()


def finish(dq_ref, ax_ref, guk_ref, guv_ref, dq_out, gl_out, gr_out, guk_out, guv_out):
    dq_out[...] = dq_ref[...]
    for s in range(NX):
        for ct in range(4):
            gl_out[0, SL * s : SL * s + SL, 128 * ct : 128 * ct + 128] = ax_ref[
                s, 16 * ct : 16 * ct + 16, :
            ].astype(F32)
        gr_out[0, 8 * s : 8 * s + 8, :] = ax_ref[s, 64:72, :].astype(F32)
    guk_out[...] = guk_ref[...]
    guv_out[...] = guv_ref[...]


def on_device(latent, rope, query, grad_out, attn_out, lse, positions, w_uk, w_uv):
    vmem = pl.BlockSpec(memory_space=pltpu.VMEM)
    hbm = pl.BlockSpec(memory_space=pltpu.HBM)
    dma = pltpu.SemaphoreType.DMA
    shapes = [
        pltpu.VMEM((1, ROWS, DL), BF16),
        pltpu.VMEM((1, DR, ROWS), BF16),
        pltpu.VMEM((1, HPD, ROWS), F32),
        pltpu.VMEM((1, NY * ROWS), jnp.int32),
        pltpu.VMEM((1, ROWS, HPD * 192), BF16),
        pltpu.VMEM((1, ROWS, HPD * DV), BF16),
        pltpu.VMEM((1, ROWS, HPD * DV), BF16),
        pltpu.VMEM((DL, 512), BF16),
        pltpu.VMEM((DL, 512), BF16),
        pltpu.VMEM((NY, 4, QR, 128), BF16),
        pltpu.VMEM((HPD, ROWS, 192), BF16),
        pltpu.VMEM((HPD, ROWS, DV), BF16),
        pltpu.VMEM((8, ROWS), F32),
        pltpu.VMEM((HPD, ROWS, 192), F32),
        pltpu.VMEM((NY, ROWS, 1024), BF16),
        pltpu.VMEM((NX, NY, GR, 128), BF16),
        pltpu.VMEM((7, NY, GR, 128), BF16),
        pltpu.VMEM((NY, GR, 128), BF16),
        pltpu.VMEM((NY, GR, 128), BF16),
        pltpu.VMEM((GR, 128), BF16),
        pltpu.VMEM((GR, 128), BF16),
        pltpu.VMEM((NX, GR, 128), BF16),
        pltpu.VMEM((2, NZ, NY, 8, 1024), BF16),
        pltpu.VMEM((NZ, NY, 8, 1024), BF16),
        pltpu.VMEM((NY, NZ, 8, 512), BF16),
        pltpu.VMEM((NZ, NY, 8, 512), BF16),
        pltpu.VMEM((NY, NZ, 8, 512), BF16),
        pltpu.VMEM((NZ, NY, 8, 512), BF16),
        pltpu.VMEM((NZ, 8, 512), BF16),
        pltpu.VMEM((NY, 8, 512), BF16),
        pltpu.VMEM((NZ, 8, 512), BF16),
        pltpu.VMEM((NY, 8, 512), BF16),
        dma((9,)),
        dma((2,)), dma((2, 4, 4)),
        dma((7,)), dma((5, 7)),
        dma((2,)), dma((2,)), dma((2,)),
        dma((2,)), dma((2,)), dma((2,)), dma((2,)), dma((2,)),
        pltpu.SemaphoreType.REGULAR((3,)), pltpu.SemaphoreType.REGULAR((3,)),
    ]
    dq, ax, guk, guv = pl.pallas_call(
        kernel,
        out_shape=(
            jax.ShapeDtypeStruct((1, ROWS, HPD * 192), BF16),
            jax.ShapeDtypeStruct((NX, GR, 128), BF16),
            jax.ShapeDtypeStruct((8, 512), BF16),
            jax.ShapeDtypeStruct((8, 512), BF16),
        ),
        in_specs=[hbm] * 9,
        out_specs=(vmem,) * 4,
        scratch_shapes=shapes,
        compiler_params=pltpu.CompilerParams(
            collective_id=0, has_side_effects=True, vmem_limit_bytes=VMEM_LIMIT
        ),
    )(
        *(
            pltpu.with_memory_space_constraint(a, pltpu.HBM)
            for a in (
                latent, jnp.transpose(rope, (0, 2, 1)), lse, positions,
                query, grad_out, attn_out, w_uk, w_uv,
            )
        )
    )
    dq, gl, gr, guk, guv = pl.pallas_call(
        finish,
        out_shape=(
            jax.ShapeDtypeStruct((1, ROWS, HPD * 192), BF16),
            jax.ShapeDtypeStruct((1, ROWS, DL), F32),
            jax.ShapeDtypeStruct((1, DR, ROWS), F32),
            jax.ShapeDtypeStruct((8, 512), BF16),
            jax.ShapeDtypeStruct((8, 512), BF16),
        ),
        in_specs=[vmem] * 4,
        out_specs=(vmem,) * 5,
        compiler_params=pltpu.CompilerParams(vmem_limit_bytes=8 * 1024 * 1024),
    )(dq, ax, guk, guv)
    return dq, gl, jnp.transpose(gr, (0, 2, 1)), guk, guv


def solution(mesh):
    return jax.shard_map(
        on_device,
        mesh=mesh,
        in_specs=(
            P("dp", "ctx", None),
            P("dp", "ctx", None),
            P("dp", "ctx", "head"),
            P("dp", "ctx", "head"),
            P("dp", "ctx", "head"),
            P("dp", "head", "ctx"),
            P("dp", None),
            P(None, "head"),
            P(None, "head"),
        ),
        out_specs=(
            P("dp", "ctx", "head"),
            P("dp", "ctx", None),
            P("dp", "ctx", None),
            P(("dp", "ctx"), "head"),
            P(("dp", "ctx"), "head"),
        ),
        check_vma=False,
    )
```

```python
import math

import jax
import jax.numpy as jnp
from jax import lax
from jax.experimental import pallas as pl
from jax.experimental.pallas import tpu as pltpu
from jax.sharding import PartitionSpec as P

DL = 512
DR = 64
DN = 128
DV = 128
HPD = 4
ROWS = 128
NY = 8
NX = 8
NZ = 4
SL = ROWS // NX
GR = 72
QR = 144
MASKED = -1e30
SCALE = 1.0 / math.sqrt(DN + DR)
VMEM_LIMIT = 40 * 1024 * 1024
MESH = pl.DeviceIdType.MESH
F32 = jnp.float32
BF16 = jnp.bfloat16

OFFS = (0, -1, 1, -2, 2, -3, 3, 4)
GROUPS = ((0, 1), (1, 3), (3, 5), (5, 7), (7, 8))


def wrap(v, n):
    return lax.rem(v + 2 * n, n)


def dot(a, b, ca, cb):
    return lax.dot_general(a, b, (((ca,), (cb,)), ((), ())), preferred_element_type=F32)


def kernel(
    lat_hbm, rope_hbm, lse_hbm, pos_hbm, q_hbm, go_hbm, ao_hbm, wuk_hbm, wuv_hbm,
    dq_out, ax_out, guk_out, guv_out,
    lat_ref, rope_ref, lse_ref, pos_ref, q_ref, go_ref, ao_ref, wuk_ref, wuv_ref,
    kv_all, qh, gh, delta, dq_acc, dkv_all, glb, xb, ysend, yrecv, zs, zr, axr,
    wgb, wgc, wa, wb, wa_in, wb_in, wa2, wb2, wa2_in, wb2_in,
    in_sem, ag_s, ag_r, x_s, x_r, y_sem, z_sem, ax_sem,
    c_sem, wy_sem, wz_sem, wy2_sem, wz2_sem, up_sem, down_sem,
):
    dp = lax.axis_index("dp")
    y = lax.axis_index("ctx")
    head = lax.axis_index("head")
    c, zl = lax.rem(dp, 2), dp // 2
    x, zh = head // 2, lax.rem(head, 2)
    z = zh * NZ + zl

    def to_y(v):
        return {"ctx": wrap(v, NY)}

    def to_x(v):
        return {"head": wrap(v, NX) * 2 + zh}

    def to_z(v):
        return {"dp": wrap(v, NZ) * 2 + c}

    other_core = {"dp": zl * 2 + (1 - c)}
    other_half = {"head": x * 2 + (1 - zh)}

    def on_line(v):
        return {"dp": lax.rem(v, NZ) * 2 + c, "head": x * 2 + v // NZ}

    def tell(sem, peer):
        pl.semaphore_signal(sem, inc=1, device_id=peer, device_id_type=MESH)

    barrier = pltpu.get_barrier_semaphore()
    peers = [to_y(y + 1), to_y(y - 1), to_x(x + 1), to_x(x - 1), to_x(x + 2), to_x(x - 2)]
    peers.append(other_core)
    for peer in peers:
        tell(barrier, peer)

    @pl.when(z < 7)
    def _():
        tell(barrier, on_line(z + 1))

    def pass_up(j):
        @pl.when((z >= 1) & (z + j <= 7))
        def _():
            tell(up_sem.at[j], on_line(z - 1))

    def take_up(j):
        @pl.when(z + j <= 6)
        def _():
            pl.semaphore_wait(up_sem.at[j], 1)

    def pass_down(j):
        @pl.when((z <= 6) & (z - j >= 0))
        def _():
            tell(down_sem.at[j - 1], on_line(z + 1))

    def take_down(j):
        @pl.when(z - j >= 1)
        def _():
            pl.semaphore_wait(down_sem.at[j - 1], 1)

    loads = []
    for i, (a, b) in enumerate(
        (
            (lat_hbm, lat_ref), (rope_hbm, rope_ref), (q_hbm, q_ref), (go_hbm, go_ref),
            (ao_hbm, ao_ref), (lse_hbm, lse_ref), (pos_hbm, pos_ref), (wuk_hbm, wuk_ref),
            (wuv_hbm, wuv_ref),
        )
    ):
        loads.append(pltpu.make_async_copy(a, b, in_sem.at[i]))
        loads[i].start()

    def copy_of(src, dst, s_sem, r_sem, device):
        return pltpu.make_async_remote_copy(
            src_ref=src, dst_ref=dst, send_sem=s_sem, recv_sem=r_sem,
            device_id=device, device_id_type=MESH,
        )

    def send(src, dst, s_sem, r_sem, device):
        copy = copy_of(src, dst, s_sem, r_sem, device)
        copy.start()
        return copy

    loads[0].wait()
    loads[1].wait()
    for t in range(4):
        for ct in range(4):
            kv_all[y, t, 32 * ct : 32 * ct + 32, :] = lat_ref[
                0, 32 * t : 32 * t + 32, 128 * ct : 128 * ct + 128
            ]
        kv_all[y, t, 128:144, :] = rope_ref[0, 16 * t : 16 * t + 16, :]

    pl.semaphore_wait(barrier, len(peers) + jnp.minimum(z, 1))

    ag = {}

    def ag_step(k, pieces=range(4)):
        for part in pieces:
            for way, sign in ((0, 1), (1, -1)):
                last = part // 2 == way
                if k == 4 and not last:
                    continue
                if k > 0:
                    ag[way, k - 1, part].wait_recv()
                if k < 3 or (k == 3 and last):
                    ref = kv_all.at[wrap(y - sign * k, NY), part]
                    ag[way, k, part] = send(
                        ref, ref, ag_s.at[way], ag_r.at[way, k, part], to_y(y + sign)
                    )

    def prepare():
        for load in loads[2:]:
            load.wait()
        for h in range(HPD):
            qh[h] = q_ref[0, :, 192 * h : 192 * h + 192]
            g = go_ref[0, :, 128 * h : 128 * h + 128]
            gh[h] = g
            prod = g.astype(F32) * ao_ref[0, :, 128 * h : 128 * h + 128].astype(F32)
            delta[h : h + 1, :] = jnp.sum(prod.T, axis=0, keepdims=True)

    def lat_of(b):
        quarters = [
            jnp.concatenate([kv_all[b, t, 32 * ct : 32 * ct + 32, :] for ct in range(4)], axis=1)
            for t in range(4)
        ]
        return jnp.concatenate(quarters, axis=0)

    def rope_of(b):
        return jnp.concatenate([kv_all[b, t, 128:144, :] for t in range(4)], axis=0).T

    def compute(group, between=None):
        pos_q = pos_ref[:, pl.ds(pl.multiple_of(y * ROWS, ROWS), ROWS)].astype(F32)
        lo, hi = GROUPS[group]
        blocks = [wrap(y + OFFS[r], NY) for r in range(lo, hi)]
        n = len(blocks)

        def joined(parts):
            return parts[0] if n == 1 else jnp.concatenate(parts, axis=0)

        masks = []
        for b in blocks:
            pos_k = pos_ref[:, pl.ds(pl.multiple_of(b * ROWS, ROWS), ROWS)].astype(F32)
            masks.append(jnp.broadcast_to(pos_k, (ROWS, ROWS)).T)
        lat = joined([lat_of(b) for b in blocks])
        rope = joined([rope_of(b) for b in blocks])
        allowed = joined(masks) <= pos_q
        keys = dot(lat, wuk_ref[...], 1, 0).astype(BF16)
        values = dot(lat, wuv_ref[...], 1, 0).astype(BF16)
        rope_grad = None
        dks, dvs = [], []
        for h in range(HPD):
            kh = jnp.concatenate([keys[:, 128 * h : 128 * h + 128], rope], axis=1)
            vh = values[:, 128 * h : 128 * h + 128]
            q, g = qh[h], gh[h]
            scores = dot(kh, q, 1, 1) * SCALE
            dots = dot(vh, g, 1, 1)
            w = jnp.exp(jnp.where(allowed, scores - lse_ref[0, h : h + 1, :], MASKED))
            sg = (w * (dots - delta[h : h + 1, :]) * SCALE).astype(BF16)
            dk = dot(sg, q, 1, 0)
            dv = dot(w.astype(BF16), g, 1, 0)
            dq = dot(sg, kh, 0, 0)
            if group == 0:
                dq_acc[h] = dq
            else:
                dq_acc[h] += dq
            part = dk[:, 128:192]
            rope_grad = part if rope_grad is None else rope_grad + part
            dks.append(dk[:, 0:128].astype(BF16))
            dvs.append(dv.astype(BF16))
            if between is not None and h == 1:
                between()
        dkn = jnp.concatenate(dks, axis=1)
        dvn = jnp.concatenate(dvs, axis=1)
        for i, b in enumerate(blocks):
            dkv_all[b, :, 0:512] = dkn[128 * i : 128 * i + 128]
            dkv_all[b, :, 512:1024] = dvn[128 * i : 128 * i + 128]
        gl = (dot(dkn, wuk_ref[...], 1, 1) + dot(dvn, wuv_ref[...], 1, 1)).astype(BF16)
        for i in range(n):
            turned = rope_grad[128 * i : 128 * i + 128].T
            for s in range(NX):
                at = 128 * i + SL * s
                for ct in range(4):
                    glb[s, lo + i, 16 * ct : 16 * ct + 16, :] = gl[
                        at : at + SL, 128 * ct : 128 * ct + 128
                    ]
                glb[s, lo + i, 64:72, :] = turned[8 * s : 8 * s + 8].astype(BF16)

    sums = {}

    def x_send(group, slot, src, step):
        lo, hi = GROUPS[group]
        sums[group, slot] = send(
            src, xb.at[slot, lo:hi], x_s.at[slot], x_r.at[group, slot], to_x(x + step)
        )

    def x_start(group):
        lo, hi = GROUPS[group]
        g = 1 - 2 * (group % 2)
        for slot, dest, step in (
            (0, -4 * g, -2 * g), (1, -3 * g, -g), (2, 3 * g, g), (3, -g, -g), (4, g, g),
        ):
            x_send(group, slot, glb.at[wrap(x + dest, NX), lo:hi], step)

    def x_middle(group):
        lo, hi = GROUPS[group]
        g = 1 - 2 * (group % 2)
        sums[group, 0].wait_recv()
        sums[group, 1].wait_recv()
        xb[0, lo:hi] = (
            xb[0, lo:hi].astype(F32)
            + xb[1, lo:hi].astype(F32)
            + glb[wrap(x - 2 * g, NX), lo:hi].astype(F32)
        ).astype(BF16)
        x_send(group, 5, xb.at[0, lo:hi], -2 * g)
        sums[group, 2].wait_recv()
        xb[2, lo:hi] = (
            xb[2, lo:hi].astype(F32) + glb[wrap(x + 2 * g, NX), lo:hi].astype(F32)
        ).astype(BF16)
        x_send(group, 6, xb.at[2, lo:hi], 2 * g)

    def x_end(group):
        lo, hi = GROUPS[group]
        total = glb[x, lo:hi].astype(F32)
        for slot in (3, 4, 5, 6):
            sums[group, slot].wait_recv()
            total += xb[slot, lo:hi].astype(F32)
        ysend[lo:hi] = total.astype(BF16)
        for r in range(lo, hi):
            if r > 0:
                send(ysend.at[r], yrecv.at[r], y_sem.at[0], y_sem.at[1], to_y(y + OFFS[r]))

    def weight_rows(i):
        lat = kv_all[:, :, 32 * i : 32 * i + 32, :].reshape(NY * ROWS, 128)
        rows = dot(lat, dkv_all[...].reshape(NY * ROWS, 1024), 0, 0)
        for half in range(2):
            wgb[half, i] = rows[64 * half : 64 * half + 64].reshape(NY, 8, 1024).astype(BF16)
        send(wgb.at[1 - c, i], wgc.at[i], c_sem.at[0], c_sem.at[1], other_core)

    def spread(src, dst, sem, n, me, to):
        order = (4, 3, 5, 2, 6, 1, 7) if n == 8 else (2, 1, 3)
        for d in order:
            send(src.at[wrap(me + d, n)], dst.at[d], sem.at[0], sem.at[1], to(me + d))

    def whole(ref, sem):
        return copy_of(ref, ref, sem.at[0], sem.at[1], other_half)

    def summed(own, got, n):
        total = own.astype(F32)
        for d in range(1, n):
            total += got[d].astype(F32)
        return total.astype(BF16)

    ag_step(0)
    pass_up(0)
    prepare()
    compute(0)
    x_start(0)
    ag_step(1)
    compute(1, lambda: ag_step(2, (0,)))
    x_start(1)
    take_up(0)
    pass_up(1)
    pass_down(1)
    ag_step(2, (1, 2, 3))
    x_middle(0)
    compute(2, lambda: ag_step(3, (0,)))
    x_start(2)
    take_up(1)
    take_down(1)
    pass_up(2)
    pass_down(2)
    ag_step(3, (1, 2, 3))
    compute(3, lambda: x_middle(1))
    x_start(3)
    take_up(2)
    take_down(2)
    pass_up(3)
    pass_down(3)
    ag_step(4)
    compute(4, lambda: x_middle(2))
    x_start(4)
    x_end(0)
    weight_rows(0)
    weight_rows(1)
    weight_rows(2)
    weight_rows(3)
    x_end(1)
    x_middle(3)
    x_middle(4)
    x_end(2)
    for h in range(HPD):
        dq_out[0, :, 192 * h : 192 * h + 192] = dq_acc[h].astype(BF16)
    take_up(3)
    take_down(3)
    x_end(3)

    whole(wgc, c_sem).wait_recv()
    for i in range(NZ):
        both = (wgb[c, i].astype(F32) + wgc[i].astype(F32)).astype(BF16)
        wa[:, i] = both[:, :, 0:512]
        wb[i] = both[:, :, 512:1024]
    spread(wb, wb_in, wz_sem, NZ, zl, to_z)
    x_end(4)
    spread(wa, wa_in, wy_sem, NY, y, to_y)

    whole(yrecv.at[1:8], y_sem).wait_recv()
    zs[...] = summed(ysend[0], yrecv, NY)
    z_copy = send(zs, zr, z_sem.at[0], z_sem.at[1], other_half)

    whole(wb_in.at[1:4], wz_sem).wait_recv()
    wb2[...] = summed(wb[zl], wb_in, NZ)
    spread(wb2, wb2_in, wy2_sem, NY, y, to_y)

    whole(wa_in.at[1:8], wy_sem).wait_recv()
    wa2[...] = summed(wa[y], wa_in, NY)
    spread(wa2, wa2_in, wz2_sem, NZ, zl, to_z)

    z_copy.wait_recv()
    axr[x] = (zs[...].astype(F32) + zr[...].astype(F32)).astype(BF16)
    for d in (4, 3, 5, 2, 6, 1, 7):
        send(axr.at[x], axr.at[x], ax_sem.at[0], ax_sem.at[1], to_x(x + d))

    whole(wb2_in.at[1:8], wy2_sem).wait_recv()
    guv_out[...] = summed(wb2[y], wb2_in, NY)
    whole(wa2_in.at[1:4], wz2_sem).wait_recv()
    guk_out[...] = summed(wa2[zl], wa2_in, NZ)
    whole(axr.at[1:8], ax_sem).wait_recv()
    ax_out[...] = axr[...]

    for way in (0, 1):
        copy_of(
            glb.at[1:8, 0:4], glb.at[1:8, 0:4], ag_s.at[way], ag_s.at[way], other_half
        ).wait_send()
    for slot in range(7):
        copy_of(xb.at[slot], xb.at[slot], x_s.at[slot], x_s.at[slot], other_half).wait_send()
    for ref, sem in (
        (wgc, c_sem), (yrecv.at[1:8], y_sem), (zr, z_sem), (axr.at[1:8], ax_sem),
        (wb_in.at[1:4], wz_sem), (wa_in.at[1:8], wy_sem),
        (wb2_in.at[1:8], wy2_sem), (wa2_in.at[1:4], wz2_sem),
    ):
        whole(ref, sem).wait_send()


def finish(dq_ref, ax_ref, guk_ref, guv_ref, dq_out, gl_out, gr_out, guk_out, guv_out):
    dq_out[...] = dq_ref[...]
    for s in range(NX):
        for ct in range(4):
            gl_out[0, SL * s : SL * s + SL, 128 * ct : 128 * ct + 128] = ax_ref[
                s, 16 * ct : 16 * ct + 16, :
            ].astype(F32)
        gr_out[0, 8 * s : 8 * s + 8, :] = ax_ref[s, 64:72, :].astype(F32)
    guk_out[...] = guk_ref[...]
    guv_out[...] = guv_ref[...]


def on_device(latent, rope, query, grad_out, attn_out, lse, positions, w_uk, w_uv):
    vmem = pl.BlockSpec(memory_space=pltpu.VMEM)
    hbm = pl.BlockSpec(memory_space=pltpu.HBM)
    dma = pltpu.SemaphoreType.DMA
    shapes = [
        pltpu.VMEM((1, ROWS, DL), BF16),
        pltpu.VMEM((1, DR, ROWS), BF16),
        pltpu.VMEM((1, HPD, ROWS), F32),
        pltpu.VMEM((1, NY * ROWS), jnp.int32),
        pltpu.VMEM((1, ROWS, HPD * 192), BF16),
        pltpu.VMEM((1, ROWS, HPD * DV), BF16),
        pltpu.VMEM((1, ROWS, HPD * DV), BF16),
        pltpu.VMEM((DL, 512), BF16),
        pltpu.VMEM((DL, 512), BF16),
        pltpu.VMEM((NY, 4, QR, 128), BF16),
        pltpu.VMEM((HPD, ROWS, 192), BF16),
        pltpu.VMEM((HPD, ROWS, DV), BF16),
        pltpu.VMEM((8, ROWS), F32),
        pltpu.VMEM((HPD, ROWS, 192), F32),
        pltpu.VMEM((NY, ROWS, 1024), BF16),
        pltpu.VMEM((NX, NY, GR, 128), BF16),
        pltpu.VMEM((7, NY, GR, 128), BF16),
        pltpu.VMEM((NY, GR, 128), BF16),
        pltpu.VMEM((NY, GR, 128), BF16),
        pltpu.VMEM((GR, 128), BF16),
        pltpu.VMEM((GR, 128), BF16),
        pltpu.VMEM((NX, GR, 128), BF16),
        pltpu.VMEM((2, NZ, NY, 8, 1024), BF16),
        pltpu.VMEM((NZ, NY, 8, 1024), BF16),
        pltpu.VMEM((NY, NZ, 8, 512), BF16),
        pltpu.VMEM((NZ, NY, 8, 512), BF16),
        pltpu.VMEM((NY, NZ, 8, 512), BF16),
        pltpu.VMEM((NZ, NY, 8, 512), BF16),
        pltpu.VMEM((NZ, 8, 512), BF16),
        pltpu.VMEM((NY, 8, 512), BF16),
        pltpu.VMEM((NZ, 8, 512), BF16),
        pltpu.VMEM((NY, 8, 512), BF16),
        dma((9,)),
        dma((2,)), dma((2, 4, 4)),
        dma((7,)), dma((5, 7)),
        dma((2,)), dma((2,)), dma((2,)),
        dma((2,)), dma((2,)), dma((2,)), dma((2,)), dma((2,)),
        pltpu.SemaphoreType.REGULAR((4,)), pltpu.SemaphoreType.REGULAR((3,)),
    ]
    dq, ax, guk, guv = pl.pallas_call(
        kernel,
        out_shape=(
            jax.ShapeDtypeStruct((1, ROWS, HPD * 192), BF16),
            jax.ShapeDtypeStruct((NX, GR, 128), BF16),
            jax.ShapeDtypeStruct((8, 512), BF16),
            jax.ShapeDtypeStruct((8, 512), BF16),
        ),
        in_specs=[hbm] * 9,
        out_specs=(vmem,) * 4,
        scratch_shapes=shapes,
        compiler_params=pltpu.CompilerParams(
            collective_id=0, has_side_effects=True, vmem_limit_bytes=VMEM_LIMIT
        ),
    )(
        *(
            pltpu.with_memory_space_constraint(a, pltpu.HBM)
            for a in (
                latent, jnp.transpose(rope, (0, 2, 1)), lse, positions,
                query, grad_out, attn_out, w_uk, w_uv,
            )
        )
    )
    dq, gl, gr, guk, guv = pl.pallas_call(
        finish,
        out_shape=(
            jax.ShapeDtypeStruct((1, ROWS, HPD * 192), BF16),
            jax.ShapeDtypeStruct((1, ROWS, DL), F32),
            jax.ShapeDtypeStruct((1, DR, ROWS), F32),
            jax.ShapeDtypeStruct((8, 512), BF16),
            jax.ShapeDtypeStruct((8, 512), BF16),
        ),
        in_specs=[vmem] * 4,
        out_specs=(vmem,) * 5,
        compiler_params=pltpu.CompilerParams(vmem_limit_bytes=8 * 1024 * 1024),
    )(dq, ax, guk, guv)
    return dq, gl, jnp.transpose(gr, (0, 2, 1)), guk, guv


def solution(mesh):
    return jax.shard_map(
        on_device,
        mesh=mesh,
        in_specs=(
            P("dp", "ctx", None),
            P("dp", "ctx", None),
            P("dp", "ctx", "head"),
            P("dp", "ctx", "head"),
            P("dp", "ctx", "head"),
            P("dp", "head", "ctx"),
            P("dp", None),
            P(None, "head"),
            P(None, "head"),
        ),
        out_specs=(
            P("dp", "ctx", "head"),
            P("dp", "ctx", None),
            P("dp", "ctx", None),
            P(("dp", "ctx"), "head"),
            P(("dp", "ctx"), "head"),
        ),
        check_vma=False,
    )
```

```python
import math

import jax
import jax.numpy as jnp
from jax import lax
from jax.experimental import pallas as pl
from jax.experimental.pallas import tpu as pltpu
from jax.sharding import PartitionSpec as P

DL = 512
DR = 64
DN = 128
DV = 128
HPD = 4
ROWS = 128
NY = 8
NX = 8
NZ = 4
SL = ROWS // NX
GR = 72
QR = 144
MASKED = -1e30
SCALE = 1.0 / math.sqrt(DN + DR)
VMEM_LIMIT = 40 * 1024 * 1024
MESH = pl.DeviceIdType.MESH
F32 = jnp.float32
BF16 = jnp.bfloat16

OFFS = (0, -1, 1, -2, 2, -3, 3, 4)
GROUPS = ((0, 1), (1, 3), (3, 5), (5, 7), (7, 8))


def wrap(v, n):
    return lax.rem(v + 2 * n, n)


def dot(a, b, ca, cb):
    return lax.dot_general(a, b, (((ca,), (cb,)), ((), ())), preferred_element_type=F32)


def kernel(
    lat_hbm, rope_hbm, lse_hbm, pos_hbm, q_hbm, go_hbm, ao_hbm, wuk_hbm, wuv_hbm,
    dq_out, ax_out, guk_out, guv_out,
    lat_ref, rope_ref, lse_ref, pos_ref, q_ref, go_ref, ao_ref, wuk_ref, wuv_ref,
    kv_all, qh, gh, delta, dq_acc, dkv_all, glb, xb, ysend, yrecv, zs, zr, axr,
    wgb, wgc, wa, wb, wa_in, wb_in, wa2, wb2, wa2_in, wb2_in,
    in_sem, ag_s, ag_r, x_s, x_r, y_sem, z_sem, ax_sem,
    c_sem, wy_sem, wz_sem, wy2_sem, wz2_sem, up_sem, down_sem,
):
    dp = lax.axis_index("dp")
    y = lax.axis_index("ctx")
    head = lax.axis_index("head")
    c, zl = lax.rem(dp, 2), dp // 2
    x, zh = head // 2, lax.rem(head, 2)
    z = zh * NZ + zl

    def to_y(v):
        return {"ctx": wrap(v, NY)}

    def to_x(v):
        return {"head": wrap(v, NX) * 2 + zh}

    def to_z(v):
        return {"dp": wrap(v, NZ) * 2 + c}

    other_core = {"dp": zl * 2 + (1 - c)}
    other_half = {"head": x * 2 + (1 - zh)}

    def on_line(v):
        return {"dp": lax.rem(v, NZ) * 2 + c, "head": x * 2 + v // NZ}

    def tell(sem, peer):
        pl.semaphore_signal(sem, inc=1, device_id=peer, device_id_type=MESH)

    barrier = pltpu.get_barrier_semaphore()
    peers = [to_y(y + 1), to_y(y - 1), to_x(x + 1), to_x(x - 1), to_x(x + 2), to_x(x - 2)]
    peers.append(other_core)
    for peer in peers:
        tell(barrier, peer)

    @pl.when(z < 7)
    def _():
        tell(barrier, on_line(z + 1))

    def pass_up(j):
        @pl.when((z >= 1) & (z + j <= 7))
        def _():
            tell(up_sem.at[j], on_line(z - 1))

    def take_up(j):
        @pl.when(z + j <= 6)
        def _():
            pl.semaphore_wait(up_sem.at[j], 1)

    def pass_down(j):
        @pl.when((z <= 6) & (z - j >= 0))
        def _():
            tell(down_sem.at[j - 1], on_line(z + 1))

    def take_down(j):
        @pl.when(z - j >= 1)
        def _():
            pl.semaphore_wait(down_sem.at[j - 1], 1)

    loads = []
    for i, (a, b) in enumerate(
        (
            (lat_hbm, lat_ref), (rope_hbm, rope_ref), (q_hbm, q_ref), (go_hbm, go_ref),
            (ao_hbm, ao_ref), (lse_hbm, lse_ref), (pos_hbm, pos_ref), (wuk_hbm, wuk_ref),
            (wuv_hbm, wuv_ref),
        )
    ):
        loads.append(pltpu.make_async_copy(a, b, in_sem.at[i]))
        loads[i].start()

    def copy_of(src, dst, s_sem, r_sem, device):
        return pltpu.make_async_remote_copy(
            src_ref=src, dst_ref=dst, send_sem=s_sem, recv_sem=r_sem,
            device_id=device, device_id_type=MESH,
        )

    def send(src, dst, s_sem, r_sem, device):
        copy = copy_of(src, dst, s_sem, r_sem, device)
        copy.start()
        return copy

    loads[0].wait()
    loads[1].wait()
    for t in range(4):
        for ct in range(4):
            kv_all[y, t, 32 * ct : 32 * ct + 32, :] = lat_ref[
                0, 32 * t : 32 * t + 32, 128 * ct : 128 * ct + 128
            ]
        kv_all[y, t, 128:144, :] = rope_ref[0, 16 * t : 16 * t + 16, :]

    pl.semaphore_wait(barrier, len(peers) + jnp.minimum(z, 1))

    ag = {}

    def ag_step(k, pieces=range(4)):
        for part in pieces:
            for way, sign in ((0, 1), (1, -1)):
                last = part // 2 == way
                if k == 4 and not last:
                    continue
                if k > 0:
                    ag[way, k - 1, part].wait_recv()
                if k < 3 or (k == 3 and last):
                    ref = kv_all.at[wrap(y - sign * k, NY), part]
                    ag[way, k, part] = send(
                        ref, ref, ag_s.at[way], ag_r.at[way, k, part], to_y(y + sign)
                    )

    def prepare():
        for load in loads[2:]:
            load.wait()
        for h in range(HPD):
            qh[h] = q_ref[0, :, 192 * h : 192 * h + 192]
            g = go_ref[0, :, 128 * h : 128 * h + 128]
            gh[h] = g
            prod = g.astype(F32) * ao_ref[0, :, 128 * h : 128 * h + 128].astype(F32)
            delta[h : h + 1, :] = jnp.sum(prod.T, axis=0, keepdims=True)

    def lat_of(b):
        quarters = [
            jnp.concatenate([kv_all[b, t, 32 * ct : 32 * ct + 32, :] for ct in range(4)], axis=1)
            for t in range(4)
        ]
        return jnp.concatenate(quarters, axis=0)

    def rope_of(b):
        return jnp.concatenate([kv_all[b, t, 128:144, :] for t in range(4)], axis=0).T

    def compute(group, between=None):
        pos_q = pos_ref[:, pl.ds(pl.multiple_of(y * ROWS, ROWS), ROWS)].astype(F32)
        lo, hi = GROUPS[group]
        blocks = [wrap(y + OFFS[r], NY) for r in range(lo, hi)]
        n = len(blocks)

        def joined(parts):
            return parts[0] if n == 1 else jnp.concatenate(parts, axis=0)

        masks = []
        for b in blocks:
            pos_k = pos_ref[:, pl.ds(pl.multiple_of(b * ROWS, ROWS), ROWS)].astype(F32)
            masks.append(jnp.broadcast_to(pos_k, (ROWS, ROWS)).T)
        lat = joined([lat_of(b) for b in blocks])
        rope = joined([rope_of(b) for b in blocks])
        allowed = joined(masks) <= pos_q
        keys = dot(lat, wuk_ref[...], 1, 0).astype(BF16)
        values = dot(lat, wuv_ref[...], 1, 0).astype(BF16)
        rope_grad = None
        dks, dvs = [], []
        for h in range(HPD):
            kh = jnp.concatenate([keys[:, 128 * h : 128 * h + 128], rope], axis=1)
            vh = values[:, 128 * h : 128 * h + 128]
            q, g = qh[h], gh[h]
            scores = dot(kh, q, 1, 1) * SCALE
            dots = dot(vh, g, 1, 1)
            w = jnp.exp(jnp.where(allowed, scores - lse_ref[0, h : h + 1, :], MASKED))
            sg = (w * (dots - delta[h : h + 1, :]) * SCALE).astype(BF16)
            dk = dot(sg, q, 1, 0)
            dv = dot(w.astype(BF16), g, 1, 0)
            dq = dot(sg, kh, 0, 0)
            if group == 0:
                dq_acc[h] = dq
            else:
                dq_acc[h] += dq
            part = dk[:, 128:192]
            rope_grad = part if rope_grad is None else rope_grad + part
            dks.append(dk[:, 0:128].astype(BF16))
            dvs.append(dv.astype(BF16))
            if between is not None and h == 1:
                between()
        dkn = jnp.concatenate(dks, axis=1)
        dvn = jnp.concatenate(dvs, axis=1)
        for i, b in enumerate(blocks):
            dkv_all[b, :, 0:512] = dkn[128 * i : 128 * i + 128]
            dkv_all[b, :, 512:1024] = dvn[128 * i : 128 * i + 128]
        gl = (dot(dkn, wuk_ref[...], 1, 1) + dot(dvn, wuv_ref[...], 1, 1)).astype(BF16)
        for i in range(n):
            turned = rope_grad[128 * i : 128 * i + 128].T
            for s in range(NX):
                at = 128 * i + SL * s
                for ct in range(4):
                    glb[s, lo + i, 16 * ct : 16 * ct + 16, :] = gl[
                        at : at + SL, 128 * ct : 128 * ct + 128
                    ]
                glb[s, lo + i, 64:72, :] = turned[8 * s : 8 * s + 8].astype(BF16)

    sums = {}

    def x_send(group, slot, src, step):
        lo, hi = GROUPS[group]
        sums[group, slot] = send(
            src, xb.at[slot, lo:hi], x_s.at[slot], x_r.at[group, slot], to_x(x + step)
        )

    def x_start(group):
        lo, hi = GROUPS[group]
        g = 1 - 2 * (group % 2)
        for slot, dest, step in (
            (0, -4 * g, -2 * g), (1, -3 * g, -g), (2, 3 * g, g), (3, -g, -g), (4, g, g),
        ):
            x_send(group, slot, glb.at[wrap(x + dest, NX), lo:hi], step)

    def x_middle(group):
        lo, hi = GROUPS[group]
        g = 1 - 2 * (group % 2)
        sums[group, 0].wait_recv()
        sums[group, 1].wait_recv()
        xb[0, lo:hi] = (
            xb[0, lo:hi].astype(F32)
            + xb[1, lo:hi].astype(F32)
            + glb[wrap(x - 2 * g, NX), lo:hi].astype(F32)
        ).astype(BF16)
        x_send(group, 5, xb.at[0, lo:hi], -2 * g)
        sums[group, 2].wait_recv()
        xb[2, lo:hi] = (
            xb[2, lo:hi].astype(F32) + glb[wrap(x + 2 * g, NX), lo:hi].astype(F32)
        ).astype(BF16)
        x_send(group, 6, xb.at[2, lo:hi], 2 * g)

    def x_end(group):
        lo, hi = GROUPS[group]
        total = glb[x, lo:hi].astype(F32)
        for slot in (3, 4, 5, 6):
            sums[group, slot].wait_recv()
            total += xb[slot, lo:hi].astype(F32)
        ysend[lo:hi] = total.astype(BF16)
        for r in range(lo, hi):
            if r > 0:
                send(ysend.at[r], yrecv.at[r], y_sem.at[0], y_sem.at[1], to_y(y + OFFS[r]))

    def weight_rows(i):
        lat = kv_all[:, :, 32 * i : 32 * i + 32, :].reshape(NY * ROWS, 128)
        rows = dot(lat, dkv_all[...].reshape(NY * ROWS, 1024), 0, 0)
        for half in range(2):
            wgb[half, i] = rows[64 * half : 64 * half + 64].reshape(NY, 8, 1024).astype(BF16)
        send(wgb.at[1 - c, i], wgc.at[i], c_sem.at[0], c_sem.at[1], other_core)

    def spread(src, dst, sem, n, me, to, order=None):
        for d in order or ((4, 3, 5, 2, 6, 1, 7) if n == 8 else (2, 1, 3)):
            send(src.at[wrap(me + d, n)], dst.at[d], sem.at[0], sem.at[1], to(me + d))

    def whole(ref, sem):
        return copy_of(ref, ref, sem.at[0], sem.at[1], other_half)

    def summed(own, got, n):
        total = own.astype(F32)
        for d in range(1, n):
            total += got[d].astype(F32)
        return total.astype(BF16)

    ag_step(0)
    pass_up(0)
    prepare()
    compute(0)
    x_start(0)
    ag_step(1)
    compute(1, lambda: ag_step(2, (0,)))
    x_start(1)
    take_up(0)
    pass_up(1)
    pass_down(1)
    ag_step(2, (1, 2, 3))
    x_middle(0)
    compute(2, lambda: ag_step(3, (0,)))
    x_start(2)
    take_up(1)
    take_down(1)
    pass_up(2)
    pass_down(2)
    ag_step(3, (1, 2, 3))
    compute(3, lambda: x_middle(1))
    x_start(3)
    take_up(2)
    take_down(2)
    pass_up(3)
    pass_down(3)
    ag_step(4)
    compute(4, lambda: x_middle(2))
    x_start(4)
    x_end(0)
    weight_rows(0)
    weight_rows(1)
    weight_rows(2)
    weight_rows(3)
    x_end(1)
    x_middle(3)
    x_middle(4)
    x_end(2)
    for h in range(HPD):
        dq_out[0, :, 192 * h : 192 * h + 192] = dq_acc[h].astype(BF16)
    take_up(3)
    take_down(3)
    x_end(3)

    whole(wgc, c_sem).wait_recv()
    for i in range(NZ):
        both = (wgb[c, i].astype(F32) + wgc[i].astype(F32)).astype(BF16)
        wa[:, i] = both[:, :, 0:512]
        wb[i] = both[:, :, 512:1024]
    spread(wb, wb_in, wz_sem, NZ, zl, to_z)
    spread(wa, wa_in, wy_sem, NY, y, to_y, (3, 2, 1))
    x_end(4)
    spread(wa, wa_in, wy_sem, NY, y, to_y, (4, 5, 6, 7))

    whole(yrecv.at[1:8], y_sem).wait_recv()
    zs[...] = summed(ysend[0], yrecv, NY)
    z_copy = send(zs, zr, z_sem.at[0], z_sem.at[1], other_half)

    whole(wb_in.at[1:4], wz_sem).wait_recv()
    wb2[...] = summed(wb[zl], wb_in, NZ)
    spread(wb2, wb2_in, wy2_sem, NY, y, to_y)

    whole(wa_in.at[1:8], wy_sem).wait_recv()
    wa2[...] = summed(wa[y], wa_in, NY)
    spread(wa2, wa2_in, wz2_sem, NZ, zl, to_z)

    z_copy.wait_recv()
    axr[x] = (zs[...].astype(F32) + zr[...].astype(F32)).astype(BF16)
    for d in (4, 3, 5, 2, 6, 1, 7):
        send(axr.at[x], axr.at[x], ax_sem.at[0], ax_sem.at[1], to_x(x + d))

    whole(wb2_in.at[1:8], wy2_sem).wait_recv()
    guv_out[...] = summed(wb2[y], wb2_in, NY)
    whole(wa2_in.at[1:4], wz2_sem).wait_recv()
    guk_out[...] = summed(wa2[zl], wa2_in, NZ)
    whole(axr.at[1:8], ax_sem).wait_recv()
    ax_out[...] = axr[...]

    for way in (0, 1):
        copy_of(
            glb.at[1:8, 0:4], glb.at[1:8, 0:4], ag_s.at[way], ag_s.at[way], other_half
        ).wait_send()
    for slot in range(7):
        copy_of(xb.at[slot], xb.at[slot], x_s.at[slot], x_s.at[slot], other_half).wait_send()
    for ref, sem in (
        (wgc, c_sem), (yrecv.at[1:8], y_sem), (zr, z_sem), (axr.at[1:8], ax_sem),
        (wb_in.at[1:4], wz_sem), (wa_in.at[1:8], wy_sem),
        (wb2_in.at[1:8], wy2_sem), (wa2_in.at[1:4], wz2_sem),
    ):
        whole(ref, sem).wait_send()


def finish(dq_ref, ax_ref, guk_ref, guv_ref, dq_out, gl_out, gr_out, guk_out, guv_out):
    dq_out[...] = dq_ref[...]
    for s in range(NX):
        for ct in range(4):
            gl_out[0, SL * s : SL * s + SL, 128 * ct : 128 * ct + 128] = ax_ref[
                s, 16 * ct : 16 * ct + 16, :
            ].astype(F32)
        gr_out[0, 8 * s : 8 * s + 8, :] = ax_ref[s, 64:72, :].astype(F32)
    guk_out[...] = guk_ref[...]
    guv_out[...] = guv_ref[...]


def on_device(latent, rope, query, grad_out, attn_out, lse, positions, w_uk, w_uv):
    vmem = pl.BlockSpec(memory_space=pltpu.VMEM)
    hbm = pl.BlockSpec(memory_space=pltpu.HBM)
    dma = pltpu.SemaphoreType.DMA
    shapes = [
        pltpu.VMEM((1, ROWS, DL), BF16),
        pltpu.VMEM((1, DR, ROWS), BF16),
        pltpu.VMEM((1, HPD, ROWS), F32),
        pltpu.VMEM((1, NY * ROWS), jnp.int32),
        pltpu.VMEM((1, ROWS, HPD * 192), BF16),
        pltpu.VMEM((1, ROWS, HPD * DV), BF16),
        pltpu.VMEM((1, ROWS, HPD * DV), BF16),
        pltpu.VMEM((DL, 512), BF16),
        pltpu.VMEM((DL, 512), BF16),
        pltpu.VMEM((NY, 4, QR, 128), BF16),
        pltpu.VMEM((HPD, ROWS, 192), BF16),
        pltpu.VMEM((HPD, ROWS, DV), BF16),
        pltpu.VMEM((8, ROWS), F32),
        pltpu.VMEM((HPD, ROWS, 192), F32),
        pltpu.VMEM((NY, ROWS, 1024), BF16),
        pltpu.VMEM((NX, NY, GR, 128), BF16),
        pltpu.VMEM((7, NY, GR, 128), BF16),
        pltpu.VMEM((NY, GR, 128), BF16),
        pltpu.VMEM((NY, GR, 128), BF16),
        pltpu.VMEM((GR, 128), BF16),
        pltpu.VMEM((GR, 128), BF16),
        pltpu.VMEM((NX, GR, 128), BF16),
        pltpu.VMEM((2, NZ, NY, 8, 1024), BF16),
        pltpu.VMEM((NZ, NY, 8, 1024), BF16),
        pltpu.VMEM((NY, NZ, 8, 512), BF16),
        pltpu.VMEM((NZ, NY, 8, 512), BF16),
        pltpu.VMEM((NY, NZ, 8, 512), BF16),
        pltpu.VMEM((NZ, NY, 8, 512), BF16),
        pltpu.VMEM((NZ, 8, 512), BF16),
        pltpu.VMEM((NY, 8, 512), BF16),
        pltpu.VMEM((NZ, 8, 512), BF16),
        pltpu.VMEM((NY, 8, 512), BF16),
        dma((9,)),
        dma((2,)), dma((2, 4, 4)),
        dma((7,)), dma((5, 7)),
        dma((2,)), dma((2,)), dma((2,)),
        dma((2,)), dma((2,)), dma((2,)), dma((2,)), dma((2,)),
        pltpu.SemaphoreType.REGULAR((4,)), pltpu.SemaphoreType.REGULAR((3,)),
    ]
    dq, ax, guk, guv = pl.pallas_call(
        kernel,
        out_shape=(
            jax.ShapeDtypeStruct((1, ROWS, HPD * 192), BF16),
            jax.ShapeDtypeStruct((NX, GR, 128), BF16),
            jax.ShapeDtypeStruct((8, 512), BF16),
            jax.ShapeDtypeStruct((8, 512), BF16),
        ),
        in_specs=[hbm] * 9,
        out_specs=(vmem,) * 4,
        scratch_shapes=shapes,
        compiler_params=pltpu.CompilerParams(
            collective_id=0, has_side_effects=True, vmem_limit_bytes=VMEM_LIMIT
        ),
    )(
        *(
            pltpu.with_memory_space_constraint(a, pltpu.HBM)
            for a in (
                latent, jnp.transpose(rope, (0, 2, 1)), lse, positions,
                query, grad_out, attn_out, w_uk, w_uv,
            )
        )
    )
    dq, gl, gr, guk, guv = pl.pallas_call(
        finish,
        out_shape=(
            jax.ShapeDtypeStruct((1, ROWS, HPD * 192), BF16),
            jax.ShapeDtypeStruct((1, ROWS, DL), F32),
            jax.ShapeDtypeStruct((1, DR, ROWS), F32),
            jax.ShapeDtypeStruct((8, 512), BF16),
            jax.ShapeDtypeStruct((8, 512), BF16),
        ),
        in_specs=[vmem] * 4,
        out_specs=(vmem,) * 5,
        compiler_params=pltpu.CompilerParams(vmem_limit_bytes=8 * 1024 * 1024),
    )(dq, ax, guk, guv)
    return dq, gl, jnp.transpose(gr, (0, 2, 1)), guk, guv


def solution(mesh):
    return jax.shard_map(
        on_device,
        mesh=mesh,
        in_specs=(
            P("dp", "ctx", None),
            P("dp", "ctx", None),
            P("dp", "ctx", "head"),
            P("dp", "ctx", "head"),
            P("dp", "ctx", "head"),
            P("dp", "head", "ctx"),
            P("dp", None),
            P(None, "head"),
            P(None, "head"),
        ),
        out_specs=(
            P("dp", "ctx", "head"),
            P("dp", "ctx", None),
            P("dp", "ctx", None),
            P(("dp", "ctx"), "head"),
            P(("dp", "ctx"), "head"),
        ),
        check_vma=False,
    )
```
